32 devices in a mesh: expert: 8 (over z, y), tensor: 4 (over x, core).
Axes of the slice: x: 2, y: 2, z: 4, core: 2. Of those that a mesh axis runs over, the one named last changes fastest.
Arguments:
- tokens: bfloat16 [1024, 2880], P(('expert', 'tensor')), may hold values from -6 to 6
- cotangent: bfloat16 [1024, 2880], P(('expert', 'tensor')), may hold values from -6 to 6
- routes: int32 [1024, 4], P(('expert', 'tensor')), may hold values from 0 to 7, all different within a row; in each aligned block of 32 rows (0 to 31, 32 to 63, ...) at most 24 rows name the same one
- combine: float32 [1024, 4], P(('expert', 'tensor')), may hold values from 0.1 to 1
- w_gate: bfloat16 [8, 2880, 1440], P('expert', None, 'tensor'), may hold values from -0.109375 to 0.109375
- w_up: bfloat16 [8, 2880, 1440], P('expert', None, 'tensor'), may hold values from -0.109375 to 0.109375
- w_down: bfloat16 [8, 1440, 2880], P('expert', 'tensor'), may hold values from -0.15625 to 0.15625
Outputs:
- token_grad: bfloat16 [1024, 2880], P(('expert', 'tensor'))
- gate_grad: bfloat16 [8, 2880, 1440], P('expert', None, 'tensor')
- up_grad: bfloat16 [8, 2880, 1440], P('expert', None, 'tensor')
- down_grad: bfloat16 [8, 1440, 2880], P('expert', 'tensor')
The draws below stay inside these ranges and needn't reach their ends.
Inputs may be any that keep to these rules, and one draw needn't show every extreme that they name: `routes`: each row names 4 different experts. Among the rows of one device no expert is named more than 24 times, and in every draw some expert is named exactly 24 times by the rows of some device.
All inputs are finite; a program needn't handle non-finite values.
Results may differ from the reference program's by a relative error of at most 0.0065.
Values may be sent and summed in bfloat16 or wider, within the bound.
A program may use at most 128 MiB of HBM per device.

```python
import math
import jax
import jax.numpy as jnp
import numpy as np
from jax import lax

D = 2880
H = 1440
TOP = 4
TOK_DEV = 32
EXPERTS = 8
CAP = 24
TOKENS = 1024
N_EXPERT = 8
N_TENSOR = 4


def levels(stream_key, shape, shards, smallest, top_value):
    level, own = 1.0, jax.random.fold_in(stream_key, 6)
    for position, shards_of in shards:
        steps = jnp.exp(jax.random.uniform(jax.random.fold_in(own, position), (shards_of,), jnp.float32, smallest / len(shards), top_value / len(shards)))
        level = level * jnp.repeat(steps, shape[position] // shards_of).reshape([-1 if axis == position else 1 for axis in range(len(shape))])
    return level


def routed_block(stream_key, own, number, rows, count, top, most, lean):
    sequence = jax.random.permutation(stream_key, count)
    packed, common = load_shares(count, rows * top, most, lean, True), load_shares(count, rows * top, most, lean, False)
    places = jnp.arange(count)

    def named(sizes, turn):
        used = int((sizes > 0).sum())
        fixed = max(1, used // 4)
        moved = fixed + (places - fixed + turn * (used - fixed)) % max(1, count - fixed)
        return jnp.zeros((count,), jnp.int32).at[sequence[jnp.where(places < fixed, places, moved)]].set(jnp.asarray(sizes, jnp.int32))

    sizes = jnp.where(number % 4 == 0, named(packed, number // 4), named(common, number - number // 4 - 1))
    mixed = jax.random.permutation(jax.random.fold_in(own, 3), count)
    giver, sink = mixed[0:count // 2 * 2:2], mixed[1:count // 2 * 2:2]
    slack = jnp.minimum(sizes[giver] - 1, most - sizes[sink]) // 2
    slack = jnp.where((giver == sequence[0]) | (sink == sequence[0]) | (sizes[sink] == 0), 0, jnp.maximum(slack, 0))
    moved = jax.random.randint(jax.random.fold_in(own, 4), (count // 2,), 0, 1 << 20) % (slack + 1)
    sizes = sizes.at[giver].add(-moved).at[sink].add(moved)
    items = jnp.searchsorted(jnp.cumsum(sizes), jnp.arange(rows * top), side="right").astype(jnp.int32)
    grid = items.reshape(top, rows).T
    grid = grid[jax.random.permutation(jax.random.fold_in(own, 1), rows)]
    turn = jax.random.randint(jax.random.fold_in(own, 2), (rows, 1), 0, top)
    return jnp.take_along_axis(grid, (jnp.arange(top)[None, :] + turn) % top, axis=1)


def load_shares(amount, total, most, lean, full):
    weights = [(1 << 20) // math.isqrt(standing ** lean) + 1 for standing in range(1, amount + 1)]
    largest = most if full else min(most, max(-(-total // amount), total * weights[0] // sum(weights)))
    least = 1 if total - largest >= amount - 1 else 0
    given, spare = [largest] + [least] * (amount - 1), total - largest - least * (amount - 1)
    while spare > 0:
        free = [i for i in range(1, amount) if given[i] < largest] or [i for i in range(1, amount) if given[i] < most]
        mass, remaining = sum([weights[i] for i in free]), spare
        for i in free:
            more = min(most - given[i], max(1, remaining * weights[i] // mass), spare)
            given[i] = given[i] + more
            spare = spare - more
    return np.array(given)


def centred(own_key, shape, deviation, bound, cuts=(), kind=jnp.bfloat16):
    factor_of = levels(own_key, shape, cuts, -0.22, 0.18) if cuts else 1.0
    array = jax.random.normal(own_key, shape, jnp.float32) * deviation * factor_of
    return jnp.minimum(jnp.maximum(array, -bound), bound).astype(kind)


def setup_inputs(seed: int = 0) -> dict:
    key_of = jax.random.split(jax.random.key(seed), 8)
    tokens = centred(key_of[0], (TOKENS, D), 1.0, 6.0, ((0, 32),))
    cotangent = centred(key_of[1], (TOKENS, D), 1.0, 6.0, ((0, 32),))
    routes_keys = jax.random.split(jax.random.fold_in(key_of[2], 1), TOKENS // TOK_DEV)
    routes_turns = jax.random.permutation(jax.random.fold_in(key_of[2], 3), TOKENS // TOK_DEV)
    routes = jax.vmap(lambda own, number: routed_block(jax.random.fold_in(key_of[2], 2), own, number, TOK_DEV, EXPERTS, TOP, CAP, 2))(routes_keys, routes_turns).reshape((TOKENS, TOP))
    combine = jnp.clip(jnp.exp(math.log(1.0) - 2.3025851 * jax.random.uniform(key_of[3], (TOKENS, TOP), jnp.float32) ** levels(key_of[3], (TOKENS, TOP), ((0, 32),), -0.2, 0.2)), 0.1, 1.0)
    w_gate = centred(key_of[4], (EXPERTS, D, H), D ** -0.5, 0.109375, ((0, 8), (2, 4)))
    w_up = centred(key_of[5], (EXPERTS, D, H), D ** -0.5, 0.109375, ((0, 8), (2, 4)))
    w_down = centred(key_of[6], (EXPERTS, H, D), H ** -0.5, 0.15625, ((0, 8), (1, 4)))
    return {"tokens": tokens, "cotangent": cotangent, "routes": routes, "combine": combine, "w_gate": w_gate, "w_up": w_up, "w_down": w_down}


def route_slots(flat, experts, cap):
    onehot = (flat[:, None] == jnp.arange(experts, dtype=jnp.int32)[None, :]).astype(jnp.int32)
    before = jnp.cumsum(onehot, axis=0) - onehot
    place = jnp.sum(before * onehot, axis=1)
    return (flat * cap + place).astype(jnp.int32)


def slot_sources(slot, count):
    target = jnp.arange(count, dtype=jnp.int32)
    match = slot[None, :] == target[:, None]
    valid = jnp.any(match, axis=1)
    order = jnp.arange(slot.shape[0], dtype=jnp.int32)
    source = jnp.sum(jnp.where(match, order[None, :], 0), axis=1).astype(jnp.int32)
    return source, valid


def reference(tokens, cotangent, routes, combine, w_gate, w_up, w_down):
    devices = N_EXPERT * N_TENSOR
    per_dev = TOK_DEV * TOP
    flat = routes.reshape(devices, per_dev).astype(jnp.int32)
    slots = jax.vmap(lambda f: route_slots(f, EXPERTS, CAP))(flat)
    source, valid = jax.vmap(lambda s: slot_sources(s, EXPERTS * CAP))(slots)
    offset = jnp.arange(devices, dtype=jnp.int32)[:, None] * per_dev
    route_index = (source + offset).astype(jnp.int32)
    route_index = route_index.reshape(devices, EXPERTS, CAP).transpose(1, 0, 2).reshape(EXPERTS, devices * CAP)
    valid = valid.reshape(devices, EXPERTS, CAP).transpose(1, 0, 2).reshape(EXPERTS, devices * CAP)
    weights_flat = combine.reshape(-1).astype(jnp.float32)

    def expert_step(items):
        e_gate, e_up, e_down, ridx, live = items
        token = (ridx // TOP).astype(jnp.int32)
        xs = jnp.where(live[:, None], tokens[token], 0).astype(tokens.dtype)
        scaled = weights_flat[ridx][:, None] * cotangent[token].astype(jnp.float32)
        dys = jnp.where(live[:, None], scaled, 0.0).astype(jnp.bfloat16)
        gate = jnp.dot(xs, e_gate, preferred_element_type=jnp.float32)
        upper = jnp.dot(xs, e_up, preferred_element_type=jnp.float32)
        sigma = jax.nn.sigmoid(gate)
        act = (gate * sigma * upper).astype(jnp.bfloat16)
        d_act = jnp.dot(dys, e_down.T, preferred_element_type=jnp.float32)
        d_down = jnp.dot(act.T, dys, preferred_element_type=jnp.float32).astype(jnp.bfloat16)
        d_upper = (d_act * gate * sigma).astype(jnp.bfloat16)
        d_gate = (d_act * upper * sigma * (1.0 + gate * (1.0 - sigma))).astype(jnp.bfloat16)
        g_grad = jnp.dot(xs.T, d_gate, preferred_element_type=jnp.float32).astype(jnp.bfloat16)
        u_grad = jnp.dot(xs.T, d_upper, preferred_element_type=jnp.float32).astype(jnp.bfloat16)
        rows = jnp.dot(d_gate, e_gate.T, preferred_element_type=jnp.float32)
        rows = rows + jnp.dot(d_upper, e_up.T, preferred_element_type=jnp.float32)
        return rows.astype(jnp.bfloat16), g_grad, u_grad, d_down

    dxs, gate_grad, up_grad, down_grad = lax.map(expert_step, (w_gate, w_up, w_down, route_index, valid))
    expert_of = flat
    place = slots - expert_of * CAP
    dev_index = jnp.arange(devices, dtype=jnp.int32)[:, None]
    row_index = (expert_of * (devices * CAP) + dev_index * CAP + place).astype(jnp.int32).reshape(-1)
    picked = dxs.reshape(EXPERTS * devices * CAP, D)[row_index].astype(jnp.float32)
    token_grad = jnp.sum(picked.reshape(TOKENS, TOP, D), axis=1).astype(jnp.bfloat16)
    return token_grad, gate_grad, up_grad, down_grad
```

```python
import jax
import jax.numpy as jnp
from jax import lax
from jax.experimental import pallas as pl
from jax.experimental.pallas import tpu as pltpu
from jax.sharding import PartitionSpec as P

MESH = pl.DeviceIdType.MESH


def route_slots(flat, experts, cap):
    onehot = (flat[:, None] == jnp.arange(experts, dtype=jnp.int32)[None, :]).astype(jnp.int32)
    before = jnp.cumsum(onehot, axis=0) - onehot
    place = jnp.sum(before * onehot, axis=1)
    return flat * cap + place


def contract_rows(left, right):
    return lax.dot_general(
        left, right, (((0,), (0,)), ((), ())), preferred_element_type=jnp.float32
    )


def contract_cols(left, right):
    return lax.dot_general(
        left, right, (((1,), (1,)), ((), ())), preferred_element_type=jnp.float32
    )


def slotted(tokens, cotangent, routes, combine, w_gate, w_up, w_down):
    tok_rows, width = tokens.shape
    top_count = routes.shape[1]
    groups = lax.axis_size("expert")
    experts = groups * w_gate.shape[0]
    cap = max(2, 3 * tok_rows * top_count // (2 * experts))
    flat = routes.reshape(-1)
    slot = route_slots(flat, experts, cap)
    target = jnp.arange(experts * cap, dtype=jnp.int32)
    match = slot[None, :] == target[:, None]
    valid = jnp.any(match, axis=1)
    order = jnp.arange(flat.shape[0], dtype=jnp.int32)
    source = jnp.sum(jnp.where(match, order[None, :], 0), axis=1)
    token = source // top_count
    send_x = jnp.where(valid[:, None], tokens[token], jnp.zeros((), tokens.dtype))
    scaled = combine.reshape(-1)[source][:, None] * cotangent[token].astype(jnp.float32)
    send_dy = jnp.where(valid[:, None], scaled, 0.0).astype(jnp.bfloat16)
    send_x = send_x.reshape(groups, cap, width)
    send_dy = send_dy.reshape(groups, cap, width)
    recv_x, recv_dy = (
        lax.all_to_all(send_x, "expert", split_axis=0, concat_axis=0, tiled=True),
        lax.all_to_all(send_dy, "expert", split_axis=0, concat_axis=0, tiled=True),
    )
    recv_x = recv_x.reshape(groups * cap, width)
    recv_dy = recv_dy.reshape(groups * cap, width)
    xs, dys = (
        lax.all_gather(recv_x, "tensor", axis=0, tiled=True),
        lax.all_gather(recv_dy, "tensor", axis=0, tiled=True),
    )
    gate_w = w_gate[0]
    up_w = w_up[0]
    down_w = w_down[0]
    gate = jnp.dot(xs, gate_w, preferred_element_type=jnp.float32)
    upper = jnp.dot(xs, up_w, preferred_element_type=jnp.float32)
    sigma = jax.nn.sigmoid(gate)
    act = (gate * sigma * upper).astype(jnp.bfloat16)
    d_act = contract_cols(dys, down_w)
    down_grad = contract_rows(act, dys).astype(jnp.bfloat16)
    d_upper = (d_act * gate * sigma).astype(jnp.bfloat16)
    d_gate = (d_act * upper * sigma * (1.0 + gate * (1.0 - sigma))).astype(jnp.bfloat16)
    gate_grad = contract_rows(xs, d_gate).astype(jnp.bfloat16)
    up_grad = contract_rows(xs, d_upper).astype(jnp.bfloat16)
    own = lax.psum_scatter(
        contract_cols(d_gate, gate_w) + contract_cols(d_upper, up_w),
        "tensor",
        scatter_dimension=0,
        tiled=True,
    )
    own = own.astype(jnp.bfloat16).reshape(groups, cap, width)
    back = lax.all_to_all(own, "expert", split_axis=0, concat_axis=0, tiled=True).reshape(
        experts * cap, width
    )
    picked = back[slot].astype(jnp.float32).reshape(tok_rows, top_count, width)
    token_grad = jnp.sum(picked, axis=1).astype(jnp.bfloat16)
    return (token_grad, gate_grad[None], up_grad[None], down_grad[None])


def place():
    e, t = lax.axis_index("expert"), lax.axis_index("tensor")
    return e // 2, lax.rem(e, 2), t // 2, lax.rem(t, 2)


def peers(depth):
    z, y, x, c = place()
    e, t = z * 2 + y, x * 2 + c
    along = [(lax.rem(z + step, depth) * 2 + y, t) for step in range(1, depth)]
    return along, (z * 2 + 1 - y, t), (e, (1 - x) * 2 + c), (e, x * 2 + 1 - c)


def greet(depth):
    along, over_y, over_x, twin = peers(depth)
    barrier = pltpu.get_barrier_semaphore()
    for device in [*along, over_y, over_x, twin]:
        pl.semaphore_signal(barrier, inc=1, device_id=device, device_id_type=MESH)
    pl.semaphore_wait(barrier, depth + 2)


def gather_kernel(depth, s_in, x_in, d_in, s_out, x_out, d_out, send_sem, recv_sem, local_sem):
    z, y, x, c = place()
    along, over_y, over_x, twin = peers(depth)
    ins, outs = (s_in, x_in, d_in), (s_out, x_out, d_out)
    sent = [[], [], []]

    def block(dz, dy, dx, dc=0):
        zz = lax.rem(z + dz, depth)
        yy, xx, cc = (1 - y if dy else y), (1 - x if dx else x), (1 - c if dc else c)
        return (zz * 2 + yy) * 4 + xx * 2 + cc

    def send(p, at, device, first=False):
        copy = pltpu.make_async_remote_copy(
            src_ref=ins[p] if first else outs[p].at[at],
            dst_ref=outs[p].at[at],
            send_sem=send_sem.at[p, len(sent[p])],
            recv_sem=recv_sem.at[p, at],
            device_id=device,
            device_id_type=MESH,
        )
        copy.start()
        sent[p].append(copy)

    def landed(p, at):
        pltpu.make_async_remote_copy(
            src_ref=ins[p],
            dst_ref=outs[p].at[at],
            send_sem=send_sem.at[p, 0],
            recv_sem=recv_sem.at[p, at],
            device_id=twin,
            device_id_type=MESH,
        ).wait_recv()

    me = block(0, 0, 0)
    keep = [pltpu.make_async_copy(ins[p], outs[p].at[me], local_sem.at[p]) for p in range(3)]
    for copy in keep:
        copy.start()
    greet(depth)
    for device in [over_y, over_x, *along, twin]:
        for p in range(3):
            send(p, me, device, True)

    def first_level(dz):
        at = block(dz, 0, 0)
        for p in range(3):
            landed(p, at)
            for device in (over_x, over_y, twin):
                send(p, at, device)

    def second_level(dz):
        by_y, by_x = block(dz, 1, 0), block(dz, 0, 1)
        for p in range(3):
            near, far, onward = (by_x, by_y, over_y) if p == 2 else (by_y, by_x, over_x)
            landed(p, near)
            send(p, near, onward)
            send(p, near, twin)
            landed(p, far)
            send(p, far, twin)

    for dz in range(1, depth):
        first_level(dz)
        second_level(dz - 1)
    second_level(depth - 1)
    for dz in range(depth):
        at = block(dz, 1, 1)
        for p in range(3):
            landed(p, at)
            send(p, at, twin)
    for dz in range(depth):
        for dy in range(2):
            for dx in range(2):
                for p in range(3):
                    landed(p, block(dz, dy, dx, 1))
    for copy in keep:
        copy.wait()
    for p in range(3):
        for copy in sent[p]:
            copy.wait_send()


def gather_all(table, tokens, cotangent):
    count = lax.axis_size("expert") * lax.axis_size("tensor")
    depth = lax.axis_size("expert") // 2
    parts = (table, tokens, cotangent)
    return pl.pallas_call(
        lambda *refs: gather_kernel(depth, *refs),
        out_shape=[jax.ShapeDtypeStruct((count, *a.shape), a.dtype) for a in parts],
        in_specs=[pl.BlockSpec(memory_space=pltpu.VMEM)] * 3,
        out_specs=[pl.BlockSpec(memory_space=pl.ANY)] * 3,
        scratch_shapes=[
            pltpu.SemaphoreType.DMA((3, count - 1)),
            pltpu.SemaphoreType.DMA((3, count)),
            pltpu.SemaphoreType.DMA((3,)),
        ],
        compiler_params=pltpu.CompilerParams(collective_id=0, has_side_effects=True),
    )(*parts)


def scatter_kernel(depth, part, out, total, twin_in, x_in, y_in, z_in, send_sem, recv_sem):
    z, y, x, c = place()
    along, over_y, over_x, twin = peers(depth)
    rows = out.shape[0] // 2
    halves = [pl.ds(0, rows), pl.ds(rows, rows)]
    sent = []

    def block(dz, dy, dx, dc=0):
        zz = lax.rem(z + dz, depth)
        yy, xx, cc = (1 - y if dy else y), (1 - x if dx else x), (1 - c if dc else c)
        return (zz * 2 + yy) * 4 + xx * 2 + cc

    def send(src, dst, device):
        copy = pltpu.make_async_remote_copy(
            src_ref=src,
            dst_ref=dst,
            send_sem=send_sem.at[len(sent)],
            recv_sem=recv_sem.at[len(sent)],
            device_id=device,
            device_id_type=MESH,
        )
        copy.start()
        sent.append(copy)
        return copy

    def add(a, b):
        return (a.astype(jnp.float32) + b.astype(jnp.float32)).astype(jnp.bfloat16)

    steps = [*range(1, depth), 0]
    corners = ((1, 1), (0, 1), (1, 0), (0, 0))
    greet(depth)
    from_twin, over, last, ends = {}, {}, {}, {}
    for dz in steps:
        for dy, dx in corners:
            i = dz * 4 + dy * 2 + dx
            from_twin[i] = send(part.at[block(dz, dy, dx, 1)], twin_in.at[i], twin)

    def merge(half, dz, other):
        over[half, dz, other].wait_recv()
        if half == 0:
            i, got = dz * 4 + other * 2, x_in.at[dz * 2 + other]
        else:
            i, got = dz * 4 + other, y_in.at[dz * 2 + other]
        total[i, halves[half]] = add(total[i, halves[half]], got[...])
        return i

    def first(dz):
        for dy, dx in corners:
            i = dz * 4 + dy * 2 + dx
            from_twin[i].wait_recv()
            total[i] = add(part[block(dz, dy, dx)], twin_in[i])
            if dx:
                over[0, dz, dy] = send(total.at[i, halves[0]], x_in.at[dz * 2 + dy], over_x)
            if dy:
                over[1, dz, dx] = send(total.at[i, halves[1]], y_in.at[dz * 2 + dx], over_y)

    def second(dz):
        i = merge(0, dz, 1)
        last[0, dz] = send(total.at[i, halves[0]], y_in.at[depth * 2 + dz], over_y)
        i = merge(1, dz, 1)
        last[1, dz] = send(total.at[i, halves[1]], x_in.at[depth * 2 + dz], over_x)

    def third(dz):
        for half in range(2):
            i = merge(half, dz, 0)
            last[half, dz].wait_recv()
            got = (x_in if half else y_in)[depth * 2 + dz]
            total[i, halves[half]] = add(total[i, halves[half]], got)
            if dz:
                ends[half, dz] = send(
                    total.at[i, halves[half]], z_in.at[half * (depth - 1) + dz - 1], along[dz - 1]
                )

    for turn in range(depth + 2):
        for stage, lag in ((first, 0), (second, 1), (third, 2)):
            if 0 <= turn - lag < depth:
                stage(steps[turn - lag])
    for half in range(2):
        value = total[0, halves[half]].astype(jnp.float32)
        for dz in range(1, depth):
            ends[half, dz].wait_recv()
            value = value + z_in[half * (depth - 1) + dz - 1].astype(jnp.float32)
        out[halves[half]] = value.astype(jnp.bfloat16)
    for copy in sent:
        copy.wait_send()


def scatter_sum(part, rows):
    width = part.shape[1]
    depth = lax.axis_size("expert") // 2
    copies = depth * 4 + 2 * (depth * 2 + depth + depth - 1)
    half = rows // 2
    return pl.pallas_call(
        lambda *refs: scatter_kernel(depth, *refs),
        out_shape=jax.ShapeDtypeStruct((rows, width), jnp.bfloat16),
        in_specs=[pl.BlockSpec(memory_space=pltpu.VMEM)],
        out_specs=pl.BlockSpec(memory_space=pltpu.VMEM),
        scratch_shapes=[
            pltpu.VMEM((depth * 4, rows, width), jnp.bfloat16),
            pltpu.VMEM((depth * 4, rows, width), jnp.bfloat16),
            pltpu.VMEM((depth * 3, half, width), jnp.bfloat16),
            pltpu.VMEM((depth * 3, half, width), jnp.bfloat16),
            pltpu.VMEM((depth * 2 - 2, half, width), jnp.bfloat16),
            pltpu.SemaphoreType.DMA((copies,)),
            pltpu.SemaphoreType.DMA((copies,)),
        ],
        compiler_params=pltpu.CompilerParams(
            collective_id=1, has_side_effects=True, vmem_limit_bytes=48 * 1024 * 1024
        ),
    )(part.reshape(-1, rows, width))


def dense(tokens, cotangent, routes, combine, w_gate, w_up, w_down):
    rows, width = tokens.shape
    experts = lax.axis_size("expert") * w_gate.shape[0]
    named = routes[:, :, None] == jnp.arange(experts, dtype=jnp.int32)[None, None, :]
    table = jnp.sum(jnp.where(named, combine[:, :, None], 0.0), axis=1).T
    table, xs, cot = gather_all(table, tokens, cotangent)
    xs = xs.reshape(-1, width)
    scale = lax.dynamic_slice_in_dim(table, lax.axis_index("expert"), 1, axis=1).reshape(-1, 1)
    dys = (scale * cot.reshape(-1, width).astype(jnp.float32)).astype(jnp.bfloat16)
    gate_w = w_gate[0]
    up_w = w_up[0]
    down_w = w_down[0]
    gate = jnp.dot(xs, gate_w, preferred_element_type=jnp.float32)
    upper = jnp.dot(xs, up_w, preferred_element_type=jnp.float32)
    sigma = jax.nn.sigmoid(gate)
    act = (gate * sigma * upper).astype(jnp.bfloat16)
    d_act = contract_cols(dys, down_w)
    d_upper = (d_act * gate * sigma).astype(jnp.bfloat16)
    d_gate = (d_act * upper * sigma * (1.0 + gate * (1.0 - sigma))).astype(jnp.bfloat16)
    part = contract_cols(d_gate, gate_w) + contract_cols(d_upper, up_w)
    token_grad = scatter_sum(part.astype(jnp.bfloat16), rows)
    down_grad = contract_rows(act, dys).astype(jnp.bfloat16)
    gate_grad = contract_rows(xs, d_gate).astype(jnp.bfloat16)
    up_grad = contract_rows(xs, d_upper).astype(jnp.bfloat16)
    return (token_grad, gate_grad[None], up_grad[None], down_grad[None])


def line_order(depth, z):
    others = sorted((abs(p - z), p) for p in range(depth) if p != z)
    return [z] + [p for _, p in others]


def pad_to(value, unit):
    return -(-value // unit) * unit


def tiles(total, size):
    full = total // size
    return full, total - full * size


def contract_first(left, right):
    return lax.dot_general(
        left, right, (((0,), (0,)), ((), ())), preferred_element_type=jnp.float32
    )


def fused_kernel(depth, experts, tok, cot, routes, comb, w_gate, w_up, w_down,
                 tg, gg, ug, dg,
                 xs, ct, dys, part, wide, g_raw, u_raw, d_raw, dgu, act_t, d_act, scl,
                 gg_buf, ug_buf, dg_buf, twin_in, total, x_in, y_in, z_in,
                 g_send, g_recv, s_send, s_recv, w_sem, o_sem):
    rows, width = tok.shape
    hid = d_raw.shape[0]
    wpad = xs.shape[1]
    hpad = d_act.shape[1]
    blocks = hpad // 128
    chunk = rows * 8
    z, y, x, c = place()
    t = x * 2 + c
    along, over_y, over_x, twin = peers(depth)
    above, below = (z * 2 + 2 + y, t), (z * 2 - 2 + y, t)
    table = [line_order(depth, zz) for zz in range(depth)]

    def plane(i):
        if i == 0:
            return z
        value = 0
        for zz in range(depth):
            value = value + jnp.where(z == zz, table[zz][i], 0)
        return value

    planes = [plane(i) for i in range(depth)]

    def block(p, dy, dx, dc=0):
        yy, xx, cc = (1 - y if dy else y), (1 - x if dx else x), (1 - c if dc else c)
        return (p * 2 + yy) * 4 + xx * 2 + cc

    def at_rows(at, count=rows):
        return pl.ds(pl.multiple_of(at * rows, rows), count)

    bufs = (xs, ct)
    sent = []
    counts = [0, 0]

    loads = [
        pltpu.make_async_copy(w_gate.at[0], g_raw, w_sem.at[0]),
        pltpu.make_async_copy(w_up.at[0], u_raw, w_sem.at[1]),
        pltpu.make_async_copy(w_down.at[0], d_raw, w_sem.at[2]),
    ]
    for load in loads:
        load.start()

    me = block(z, 0, 0)
    lane = lax.broadcasted_iota(jnp.int32, (rows, 128), 1)
    first_lane = width - (wpad - 128)
    owner = lax.rem(lane - first_lane + experts, experts)
    named = jnp.zeros((rows, 128), jnp.float32)
    for k in range(routes.shape[1]):
        named = named + jnp.where(routes[:, k : k + 1] == owner, comb[:, k : k + 1], 0.0)
    high = named.astype(jnp.bfloat16).astype(jnp.float32)
    mid = (named - high).astype(jnp.bfloat16).astype(jnp.float32)
    low = named - high - mid
    piece = jnp.where(lane < first_lane + experts, high, jnp.where(lane < first_lane + 2 * experts, mid, low))
    piece = jnp.where(lane < first_lane + 3 * experts, piece, 0.0)
    tail = jnp.concatenate(
        [tok[:, wpad - 128 : width].astype(jnp.float32), jnp.zeros((rows, wpad - width), jnp.float32)], axis=1
    )
    xs[at_rows(me), : wpad - 128] = tok[:, : wpad - 128]
    xs[at_rows(me), wpad - 128 :] = jnp.where(lane < first_lane, tail, piece).astype(jnp.bfloat16)
    ct[at_rows(me), :] = cot[...]
    greet(depth)

    def send(q, at, device, cond=None):
        copy = pltpu.make_async_remote_copy(
            src_ref=bufs[q].at[at_rows(at)],
            dst_ref=bufs[q].at[at_rows(at)],
            send_sem=g_send.at[q, counts[q]],
            recv_sem=g_recv.at[q, at],
            device_id=device,
            device_id_type=MESH,
        )
        counts[q] += 1
        if cond is None:
            copy.start()
        else:
            pl.when(cond)(copy.start)
        sent.append((copy, cond))

    def landed(q, at):
        pltpu.make_async_remote_copy(
            src_ref=bufs[q].at[at_rows(at)],
            dst_ref=bufs[q].at[at_rows(at)],
            send_sem=g_send.at[q, 0],
            recv_sem=g_recv.at[q, at],
            device_id=twin,
            device_id_type=MESH,
        ).wait_recv()

    def send_z(q, i, at):
        if i == 0:
            send(q, at, above, z < depth - 1)
            send(q, at, below, z > 0)
        else:
            up = planes[i] < z
            zz = jnp.where(up, z + 1, z - 1)
            onward = jnp.where(up, z < depth - 1, z > 0)
            send(q, at, (zz * 2 + y, t), onward)

    def first(i):
        at = block(planes[i], 0, 0)
        for q in range(2):
            if i:
                landed(q, at)
            send_z(q, i, at)
            send(q, at, over_x)
            send(q, at, over_y)
            send(q, at, twin)

    def second(i):
        by_y, by_x = block(planes[i], 1, 0), block(planes[i], 0, 1)
        for q in range(2):
            near, far, onward = (by_x, by_y, over_y) if q else (by_y, by_x, over_x)
            landed(q, near)
            if i == 0 or q not in ZDIAG:
                send(q, near, onward)
            send(q, near, twin)
            landed(q, far)
            send(q, far, twin)

    def third(i):
        at = block(planes[i], 1, 1)
        for q in range(2):
            landed(q, at)
            if q in ZDIAG:
                send_z(q, i, at)
            send(q, at, twin)

    def fourth(i):
        for dy in range(2):
            for dx in range(2):
                for q in range(2):
                    landed(q, block(planes[i], dy, dx, 1))

    def prepare():
        for load in loads:
            load.wait()
        wide[width:, :] = jnp.zeros((wpad - width, wide.shape[1]), jnp.bfloat16)
        for raw, side in ((g_raw, 0), (u_raw, 1)):
            for j in range(blocks):
                to = 256 * j + 128 * side
                live = min(128, hid - 128 * j)
                if live < 128:
                    wide[:width, to : to + 128] = jnp.zeros((width, 128), jnp.bfloat16)
                wide[:width, to : to + live] = raw[:, 128 * j : 128 * j + live]
        d_act[...] = jnp.zeros(d_act.shape, jnp.float32)

    def compute(i):
        r0 = pl.multiple_of(planes[i] * chunk, chunk)
        here = pl.ds(r0, chunk)
        spot = lax.broadcasted_iota(jnp.int32, (chunk, 128), 1) - first_lane
        e = lax.axis_index("expert")
        mine = (spot == e) | (spot == e + experts) | (spot == e + 2 * experts)
        scale = jnp.sum(jnp.where(mine, xs[here, wpad - 128 :].astype(jnp.float32), 0.0), axis=1, keepdims=True)
        scl[...] = jnp.broadcast_to(scale, (chunk, 128))

        def scaled(k, _):
            at = pl.ds(pl.multiple_of(r0 + k * 16, 16), 16)
            by = scl[pl.ds(pl.multiple_of(k * 16, 16), 16), 0:1]
            dys[at, :] = (by * ct[at, :].astype(jnp.float32)).astype(jnp.bfloat16)
            return 0

        lax.fori_loop(0, chunk // 16, scaled, 0)
        d_act[:, :hid] = contract_cols(dys[here, :], d_raw[...])

        def gates(j, _):
            cols = pl.ds(pl.multiple_of(j * 256, 256), 256)
            both = jnp.dot(xs[here, :], wide[:, cols], preferred_element_type=jnp.float32)
            gate, upper = both[:, :128], both[:, 128:]
            da = d_act[:, pl.ds(pl.multiple_of(j * 128, 128), 128)]
            sigma = jax.nn.sigmoid(gate)
            act = gate * sigma * upper
            act_t[pl.ds(pl.multiple_of(j * 128, 128), 128), here] = act.T.astype(jnp.bfloat16)
            dgu[here, pl.ds(pl.multiple_of(j * 256, 256), 128)] = (
                da * upper * sigma * (1.0 + gate * (1.0 - sigma))
            ).astype(jnp.bfloat16)
            dgu[here, pl.ds(pl.multiple_of(j * 256 + 128, 128), 128)] = (da * gate * sigma).astype(jnp.bfloat16)
            return 0

        lax.fori_loop(0, blocks, gates, 0)
        size = 512
        full, rest = tiles(width, size)

        def back(k, _):
            cols = pl.ds(pl.multiple_of(k * size, size), size)
            part[here, cols] = contract_cols(dgu[here, :], wide[cols, :]).astype(jnp.bfloat16)
            return 0

        lax.fori_loop(0, full, back, 0)
        if rest:
            part[here, full * size : width] = contract_cols(
                dgu[here, :], wide[full * size : width, :]
            ).astype(jnp.bfloat16)

    half = rows // 2
    halves = [pl.ds(0, half), pl.ds(half, half)]
    ssent = []

    def ssend(src, dst, device, recv):
        copy = pltpu.make_async_remote_copy(
            src_ref=src,
            dst_ref=dst,
            send_sem=s_send.at[len(ssent)],
            recv_sem=s_recv.at[recv] if recv is not None else s_recv.at[len(ssent)],
            device_id=device,
            device_id_type=MESH,
        )
        copy.start()
        ssent.append(copy)
        return copy

    def add(a, b):
        return (a.astype(jnp.float32) + b.astype(jnp.float32)).astype(jnp.bfloat16)

    corners = ((1, 1), (0, 1), (1, 0), (0, 0))
    from_twin, over, last = {}, {}, {}
    z_base = depth * 10

    def s0(i):
        for dy, dx in corners:
            k = i * 4 + dy * 2 + dx
            from_twin[k] = ssend(part.at[at_rows(block(planes[i], dy, dx, 1))], twin_in.at[k], twin, k)

    def merge(h, i, other):
        over[h, i, other].wait_recv()
        if h == 0:
            k, got = i * 4 + other * 2, x_in.at[i * 2 + other]
        else:
            k, got = i * 4 + other, y_in.at[i * 2 + other]
        total[k, halves[h]] = add(total[k, halves[h]], got[...])
        return k

    def s1(i):
        for dy, dx in corners:
            k = i * 4 + dy * 2 + dx
            from_twin[k].wait_recv()
            total[k] = add(part[at_rows(block(planes[i], dy, dx)), :], twin_in[k])
            if dx:
                over[0, i, dy] = ssend(total.at[k, halves[0]], x_in.at[i * 2 + dy], over_x, depth * 4 + i * 2 + dy)
            if dy:
                over[1, i, dx] = ssend(total.at[k, halves[1]], y_in.at[i * 2 + dx], over_y, depth * 6 + i * 2 + dx)

    def s2(i):
        k = merge(0, i, 1)
        last[0, i] = ssend(total.at[k, halves[0]], y_in.at[depth * 2 + i], over_y, depth * 8 + i)
        k = merge(1, i, 1)
        last[1, i] = ssend(total.at[k, halves[1]], x_in.at[depth * 2 + i], over_x, depth * 9 + i)

    def s3(i):
        for h in range(2):
            k = merge(h, i, 0)
            last[h, i].wait_recv()
            got = (x_in if h else y_in)[depth * 2 + i]
            total[k, halves[h]] = add(total[k, halves[h]], got)
            if i:
                ssend(
                    total.at[k, halves[h]], z_in.at[h * depth + z], (planes[i] * 2 + y, t), z_base + h * depth + z
                )

    def finish():
        for h in range(2):
            value = total[0, halves[h]].astype(jnp.float32)
            for step in range(1, depth):
                zz = lax.rem(z + step, depth)
                at = h * depth + zz
                pltpu.make_async_remote_copy(
                    src_ref=total.at[0, halves[h]],
                    dst_ref=z_in.at[at],
                    send_sem=s_send.at[0],
                    recv_sem=s_recv.at[z_base + at],
                    device_id=twin,
                    device_id_type=MESH,
                ).wait_recv()
                value = value + z_in[at].astype(jnp.float32)
            tg[halves[h], :] = value.astype(jnp.bfloat16)

    msize = 384
    mfull, mrest = tiles(wpad, msize)

    def wide_tile(start, size, valid):
        out = contract_first(xs[:, pl.ds(start, size)], dgu[...])
        for j in range(blocks):
            live = min(128, hid - 128 * j)
            for buf, side in ((gg_buf, 0), (ug_buf, 1)):
                at = 256 * j + 128 * side
                buf[pl.ds(start, valid), 128 * j : 128 * j + live] = out[:valid, at : at + live].astype(jnp.bfloat16)

    def wide_grads(lo, hi):
        def body(k, _):
            wide_tile(pl.multiple_of(k * msize, msize), msize, msize)
            return 0

        lax.fori_loop(lo, hi, body, 0)

    def wide_rest():
        if mrest:
            wide_tile(mfull * msize, mrest, width - mfull * msize)
        for q, (src, dst) in enumerate(((gg_buf, gg), (ug_buf, ug))):
            outs.append(pltpu.make_async_copy(src, dst.at[0], o_sem.at[q]))
            outs[-1].start()

    nsize = 512
    nfull, nrest = tiles(width, nsize)
    outs = []

    def down_grads():
        def body(k, _):
            cols = pl.ds(pl.multiple_of(k * nsize, nsize), nsize)
            dg_buf[:, cols] = jnp.dot(
                act_t[...], dys[:, cols], preferred_element_type=jnp.float32
            )[:hid].astype(jnp.bfloat16)
            return 0

        lax.fori_loop(0, nfull, body, 0)
        if nrest:
            dg_buf[:, nfull * nsize : width] = jnp.dot(
                act_t[...], dys[:, nfull * nsize : width], preferred_element_type=jnp.float32
            )[:hid].astype(jnp.bfloat16)
        outs.append(pltpu.make_async_copy(dg_buf, dg.at[0], o_sem.at[2]))
        outs[-1].start()

    first(0)
    prepare()
    for i in range(depth):
        if i == 0 and depth > 1:
            first(1)
            second(0)
        if i == 0 and depth == 1:
            second(0)
        third(i)
        if i + 2 < depth:
            first(i + 2)
        if i + 1 < depth:
            second(i + 1)
        for lag, stage in ((1, s1), (2, s2), (3, s3)):
            if i >= lag:
                stage(i - lag)
        fourth(i)
        compute(i)
        s0(i)
    if depth > 1:
        s2(depth - 2)
    if depth > 2:
        s3(depth - 3)
    s1(depth - 1)
    down_grads()
    if depth > 1:
        s3(depth - 2)
    s2(depth - 1)
    wide_grads(0, mfull // 2)
    s3(depth - 1)
    wide_grads(mfull // 2, mfull)
    wide_rest()
    finish()
    for copy, cond in sent:
        if cond is None:
            copy.wait_send()
        else:
            pl.when(cond)(copy.wait_send)
    for copy in ssent:
        copy.wait_send()
    for copy in outs:
        copy.wait()


ZDIAG = (0, 1)


def fused(tokens, cotangent, routes, combine, w_gate, w_up, w_down):
    rows, width = tokens.shape
    hid = w_gate.shape[2]
    groups = lax.axis_size("expert")
    depth = groups // 2
    wpad, hpad = pad_to(width, 128), pad_to(hid, 128)
    count = groups * 4
    everyone = count * rows
    half = rows // 2
    copies = depth * 4 + depth * 4 + depth * 2 + 2 * (depth - 1)
    vmem = pl.BlockSpec(memory_space=pltpu.VMEM)
    hbm = pl.BlockSpec(memory_space=pl.ANY)
    bf16, f32 = jnp.bfloat16, jnp.float32
    return pl.pallas_call(
        lambda *refs: fused_kernel(depth, groups, *refs),
        out_shape=[
            jax.ShapeDtypeStruct(tokens.shape, bf16),
            jax.ShapeDtypeStruct(w_gate.shape, bf16),
            jax.ShapeDtypeStruct(w_up.shape, bf16),
            jax.ShapeDtypeStruct(w_down.shape, bf16),
        ],
        in_specs=[vmem] * 4 + [hbm] * 3,
        out_specs=[vmem] + [hbm] * 3,
        scratch_shapes=[
            pltpu.VMEM((everyone, wpad), bf16),
            pltpu.VMEM((everyone, width), bf16),
            pltpu.VMEM((everyone, width), bf16),
            pltpu.VMEM((everyone, width), bf16),
            pltpu.VMEM((wpad, 2 * hpad), bf16),
            pltpu.VMEM((width, hid), bf16),
            pltpu.VMEM((width, hid), bf16),
            pltpu.VMEM((hid, width), bf16),
            pltpu.VMEM((everyone, 2 * hpad), bf16),
            pltpu.VMEM((hpad, everyone), bf16),
            pltpu.VMEM((rows * 8, hpad), f32),
            pltpu.VMEM((rows * 8, 128), f32),
            pltpu.VMEM((width, hid), bf16),
            pltpu.VMEM((width, hid), bf16),
            pltpu.VMEM((hid, width), bf16),
            pltpu.VMEM((depth * 4, rows, width), bf16),
            pltpu.VMEM((depth * 4, rows, width), bf16),
            pltpu.VMEM((depth * 3, half, width), bf16),
            pltpu.VMEM((depth * 3, half, width), bf16),
            pltpu.VMEM((depth * 2, half, width), bf16),
            pltpu.SemaphoreType.DMA((2, depth * 9 + 2)),
            pltpu.SemaphoreType.DMA((2, count)),
            pltpu.SemaphoreType.DMA((copies,)),
            pltpu.SemaphoreType.DMA((depth * 12,)),
            pltpu.SemaphoreType.DMA((3,)),
            pltpu.SemaphoreType.DMA((3,)),
        ],
        compiler_params=pltpu.CompilerParams(
            collective_id=0, has_side_effects=True, vmem_limit_bytes=67_043_328
        ),
    )(tokens, cotangent, routes, combine, w_gate, w_up, w_down)


def on_device(tokens, cotangent, routes, combine, w_gate, w_up, w_down):
    groups, shards = lax.axis_size("expert"), lax.axis_size("tensor")
    rows, top_count = routes.shape
    few = w_gate.shape[0] == 1 and groups <= 2 * top_count
    plan = slotted
    if few and shards == 4 and groups % 2 == 0 and rows % 32 == 0:
        plan = fused if -tokens.shape[1] % 128 >= 3 * groups else dense
    return plan(tokens, cotangent, routes, combine, w_gate, w_up, w_down)


def solution(mesh):
    in_specs = (
        P(("expert", "tensor"), None),
        P(("expert", "tensor"), None),
        P(("expert", "tensor"), None),
        P(("expert", "tensor"), None),
        P("expert", None, "tensor"),
        P("expert", None, "tensor"),
        P("expert", "tensor", None),
    )
    out_specs = (
        P(("expert", "tensor"), None),
        P("expert", None, "tensor"),
        P("expert", None, "tensor"),
        P("expert", "tensor", None),
    )
    return jax.shard_map(
        on_device, mesh=mesh, in_specs=in_specs, out_specs=out_specs, check_vma=False
    )
```

```python
import functools

import jax
import jax.numpy as jnp
from jax import lax
from jax.experimental import pallas as pl
from jax.experimental.pallas import tpu as pltpu
from jax.sharding import PartitionSpec as P

MESH = pl.DeviceIdType.MESH


def route_slots(flat, experts, cap):
    onehot = (flat[:, None] == jnp.arange(experts, dtype=jnp.int32)[None, :]).astype(jnp.int32)
    before = jnp.cumsum(onehot, axis=0) - onehot
    place = jnp.sum(before * onehot, axis=1)
    return flat * cap + place


def contract_rows(left, right):
    return lax.dot_general(
        left, right, (((0,), (0,)), ((), ())), preferred_element_type=jnp.float32
    )


def contract_cols(left, right):
    return lax.dot_general(
        left, right, (((1,), (1,)), ((), ())), preferred_element_type=jnp.float32
    )


def slotted(tokens, cotangent, routes, combine, w_gate, w_up, w_down):
    tok_rows, width = tokens.shape
    top_count = routes.shape[1]
    groups = lax.axis_size("expert")
    experts = groups * w_gate.shape[0]
    cap = max(2, 3 * tok_rows * top_count // (2 * experts))
    flat = routes.reshape(-1)
    slot = route_slots(flat, experts, cap)
    target = jnp.arange(experts * cap, dtype=jnp.int32)
    match = slot[None, :] == target[:, None]
    valid = jnp.any(match, axis=1)
    order = jnp.arange(flat.shape[0], dtype=jnp.int32)
    source = jnp.sum(jnp.where(match, order[None, :], 0), axis=1)
    token = source // top_count
    send_x = jnp.where(valid[:, None], tokens[token], jnp.zeros((), tokens.dtype))
    scaled = combine.reshape(-1)[source][:, None] * cotangent[token].astype(jnp.float32)
    send_dy = jnp.where(valid[:, None], scaled, 0.0).astype(jnp.bfloat16)
    send_x = send_x.reshape(groups, cap, width)
    send_dy = send_dy.reshape(groups, cap, width)
    recv_x, recv_dy = (
        lax.all_to_all(send_x, "expert", split_axis=0, concat_axis=0, tiled=True),
        lax.all_to_all(send_dy, "expert", split_axis=0, concat_axis=0, tiled=True),
    )
    recv_x = recv_x.reshape(groups * cap, width)
    recv_dy = recv_dy.reshape(groups * cap, width)
    xs, dys = (
        lax.all_gather(recv_x, "tensor", axis=0, tiled=True),
        lax.all_gather(recv_dy, "tensor", axis=0, tiled=True),
    )
    gate_w = w_gate[0]
    up_w = w_up[0]
    down_w = w_down[0]
    gate = jnp.dot(xs, gate_w, preferred_element_type=jnp.float32)
    upper = jnp.dot(xs, up_w, preferred_element_type=jnp.float32)
    sigma = jax.nn.sigmoid(gate)
    act = (gate * sigma * upper).astype(jnp.bfloat16)
    d_act = contract_cols(dys, down_w)
    down_grad = contract_rows(act, dys).astype(jnp.bfloat16)
    d_upper = (d_act * gate * sigma).astype(jnp.bfloat16)
    d_gate = (d_act * upper * sigma * (1.0 + gate * (1.0 - sigma))).astype(jnp.bfloat16)
    gate_grad = contract_rows(xs, d_gate).astype(jnp.bfloat16)
    up_grad = contract_rows(xs, d_upper).astype(jnp.bfloat16)
    own = lax.psum_scatter(
        contract_cols(d_gate, gate_w) + contract_cols(d_upper, up_w),
        "tensor",
        scatter_dimension=0,
        tiled=True,
    )
    own = own.astype(jnp.bfloat16).reshape(groups, cap, width)
    back = lax.all_to_all(own, "expert", split_axis=0, concat_axis=0, tiled=True).reshape(
        experts * cap, width
    )
    picked = back[slot].astype(jnp.float32).reshape(tok_rows, top_count, width)
    token_grad = jnp.sum(picked, axis=1).astype(jnp.bfloat16)
    return (token_grad, gate_grad[None], up_grad[None], down_grad[None])


def place():
    e, t = lax.axis_index("expert"), lax.axis_index("tensor")
    return e // 2, lax.rem(e, 2), t // 2, lax.rem(t, 2)


def peers(depth):
    z, y, x, c = place()
    e, t = z * 2 + y, x * 2 + c
    along = [(lax.rem(z + step, depth) * 2 + y, t) for step in range(1, depth)]
    return along, (z * 2 + 1 - y, t), (e, (1 - x) * 2 + c), (e, x * 2 + 1 - c)


def greet(depth):
    along, over_y, over_x, twin = peers(depth)
    barrier = pltpu.get_barrier_semaphore()
    for device in [*along, over_y, over_x, twin]:
        pl.semaphore_signal(barrier, inc=1, device_id=device, device_id_type=MESH)
    pl.semaphore_wait(barrier, depth + 2)


def gather_kernel(depth, s_in, x_in, d_in, s_out, x_out, d_out, send_sem, recv_sem, local_sem):
    z, y, x, c = place()
    along, over_y, over_x, twin = peers(depth)
    ins, outs = (s_in, x_in, d_in), (s_out, x_out, d_out)
    sent = [[], [], []]

    def block(dz, dy, dx, dc=0):
        zz = lax.rem(z + dz, depth)
        yy, xx, cc = (1 - y if dy else y), (1 - x if dx else x), (1 - c if dc else c)
        return (zz * 2 + yy) * 4 + xx * 2 + cc

    def send(p, at, device, first=False):
        copy = pltpu.make_async_remote_copy(
            src_ref=ins[p] if first else outs[p].at[at],
            dst_ref=outs[p].at[at],
            send_sem=send_sem.at[p, len(sent[p])],
            recv_sem=recv_sem.at[p, at],
            device_id=device,
            device_id_type=MESH,
        )
        copy.start()
        sent[p].append(copy)

    def landed(p, at):
        pltpu.make_async_remote_copy(
            src_ref=ins[p],
            dst_ref=outs[p].at[at],
            send_sem=send_sem.at[p, 0],
            recv_sem=recv_sem.at[p, at],
            device_id=twin,
            device_id_type=MESH,
        ).wait_recv()

    me = block(0, 0, 0)
    keep = [pltpu.make_async_copy(ins[p], outs[p].at[me], local_sem.at[p]) for p in range(3)]
    for copy in keep:
        copy.start()
    greet(depth)
    for device in [over_y, over_x, *along, twin]:
        for p in range(3):
            send(p, me, device, True)

    def first_level(dz):
        at = block(dz, 0, 0)
        for p in range(3):
            landed(p, at)
            for device in (over_x, over_y, twin):
                send(p, at, device)

    def second_level(dz):
        by_y, by_x = block(dz, 1, 0), block(dz, 0, 1)
        for p in range(3):
            near, far, onward = (by_x, by_y, over_y) if p == 2 else (by_y, by_x, over_x)
            landed(p, near)
            send(p, near, onward)
            send(p, near, twin)
            landed(p, far)
            send(p, far, twin)

    for dz in range(1, depth):
        first_level(dz)
        second_level(dz - 1)
    second_level(depth - 1)
    for dz in range(depth):
        at = block(dz, 1, 1)
        for p in range(3):
            landed(p, at)
            send(p, at, twin)
    for dz in range(depth):
        for dy in range(2):
            for dx in range(2):
                for p in range(3):
                    landed(p, block(dz, dy, dx, 1))
    for copy in keep:
        copy.wait()
    for p in range(3):
        for copy in sent[p]:
            copy.wait_send()


def gather_all(table, tokens, cotangent):
    count = lax.axis_size("expert") * lax.axis_size("tensor")
    depth = lax.axis_size("expert") // 2
    parts = (table, tokens, cotangent)
    return pl.pallas_call(
        lambda *refs: gather_kernel(depth, *refs),
        out_shape=[jax.ShapeDtypeStruct((count, *a.shape), a.dtype) for a in parts],
        in_specs=[pl.BlockSpec(memory_space=pltpu.VMEM)] * 3,
        out_specs=[pl.BlockSpec(memory_space=pl.ANY)] * 3,
        scratch_shapes=[
            pltpu.SemaphoreType.DMA((3, count - 1)),
            pltpu.SemaphoreType.DMA((3, count)),
            pltpu.SemaphoreType.DMA((3,)),
        ],
        compiler_params=pltpu.CompilerParams(collective_id=0, has_side_effects=True),
    )(*parts)


def scatter_kernel(depth, part, out, total, twin_in, x_in, y_in, z_in, send_sem, recv_sem):
    z, y, x, c = place()
    along, over_y, over_x, twin = peers(depth)
    rows = out.shape[0] // 2
    halves = [pl.ds(0, rows), pl.ds(rows, rows)]
    sent = []

    def block(dz, dy, dx, dc=0):
        zz = lax.rem(z + dz, depth)
        yy, xx, cc = (1 - y if dy else y), (1 - x if dx else x), (1 - c if dc else c)
        return (zz * 2 + yy) * 4 + xx * 2 + cc

    def send(src, dst, device):
        copy = pltpu.make_async_remote_copy(
            src_ref=src,
            dst_ref=dst,
            send_sem=send_sem.at[len(sent)],
            recv_sem=recv_sem.at[len(sent)],
            device_id=device,
            device_id_type=MESH,
        )
        copy.start()
        sent.append(copy)
        return copy

    def add(a, b):
        return (a.astype(jnp.float32) + b.astype(jnp.float32)).astype(jnp.bfloat16)

    steps = [*range(1, depth), 0]
    corners = ((1, 1), (0, 1), (1, 0), (0, 0))
    greet(depth)
    from_twin, over, last, ends = {}, {}, {}, {}
    for dz in steps:
        for dy, dx in corners:
            i = dz * 4 + dy * 2 + dx
            from_twin[i] = send(part.at[block(dz, dy, dx, 1)], twin_in.at[i], twin)

    def merge(half, dz, other):
        over[half, dz, other].wait_recv()
        if half == 0:
            i, got = dz * 4 + other * 2, x_in.at[dz * 2 + other]
        else:
            i, got = dz * 4 + other, y_in.at[dz * 2 + other]
        total[i, halves[half]] = add(total[i, halves[half]], got[...])
        return i

    def first(dz):
        for dy, dx in corners:
            i = dz * 4 + dy * 2 + dx
            from_twin[i].wait_recv()
            total[i] = add(part[block(dz, dy, dx)], twin_in[i])
            if dx:
                over[0, dz, dy] = send(total.at[i, halves[0]], x_in.at[dz * 2 + dy], over_x)
            if dy:
                over[1, dz, dx] = send(total.at[i, halves[1]], y_in.at[dz * 2 + dx], over_y)

    def second(dz):
        i = merge(0, dz, 1)
        last[0, dz] = send(total.at[i, halves[0]], y_in.at[depth * 2 + dz], over_y)
        i = merge(1, dz, 1)
        last[1, dz] = send(total.at[i, halves[1]], x_in.at[depth * 2 + dz], over_x)

    def third(dz):
        for half in range(2):
            i = merge(half, dz, 0)
            last[half, dz].wait_recv()
            got = (x_in if half else y_in)[depth * 2 + dz]
            total[i, halves[half]] = add(total[i, halves[half]], got)
            if dz:
                ends[half, dz] = send(
                    total.at[i, halves[half]], z_in.at[half * (depth - 1) + dz - 1], along[dz - 1]
                )

    for turn in range(depth + 2):
        for stage, lag in ((first, 0), (second, 1), (third, 2)):
            if 0 <= turn - lag < depth:
                stage(steps[turn - lag])
    for half in range(2):
        value = total[0, halves[half]].astype(jnp.float32)
        for dz in range(1, depth):
            ends[half, dz].wait_recv()
            value = value + z_in[half * (depth - 1) + dz - 1].astype(jnp.float32)
        out[halves[half]] = value.astype(jnp.bfloat16)
    for copy in sent:
        copy.wait_send()


def scatter_sum(part, rows):
    width = part.shape[1]
    depth = lax.axis_size("expert") // 2
    copies = depth * 4 + 2 * (depth * 2 + depth + depth - 1)
    half = rows // 2
    return pl.pallas_call(
        lambda *refs: scatter_kernel(depth, *refs),
        out_shape=jax.ShapeDtypeStruct((rows, width), jnp.bfloat16),
        in_specs=[pl.BlockSpec(memory_space=pltpu.VMEM)],
        out_specs=pl.BlockSpec(memory_space=pltpu.VMEM),
        scratch_shapes=[
            pltpu.VMEM((depth * 4, rows, width), jnp.bfloat16),
            pltpu.VMEM((depth * 4, rows, width), jnp.bfloat16),
            pltpu.VMEM((depth * 3, half, width), jnp.bfloat16),
            pltpu.VMEM((depth * 3, half, width), jnp.bfloat16),
            pltpu.VMEM((depth * 2 - 2, half, width), jnp.bfloat16),
            pltpu.SemaphoreType.DMA((copies,)),
            pltpu.SemaphoreType.DMA((copies,)),
        ],
        compiler_params=pltpu.CompilerParams(
            collective_id=1, has_side_effects=True, vmem_limit_bytes=48 * 1024 * 1024
        ),
    )(part.reshape(-1, rows, width))


def dense(tokens, cotangent, routes, combine, w_gate, w_up, w_down):
    rows, width = tokens.shape
    experts = lax.axis_size("expert") * w_gate.shape[0]
    named = routes[:, :, None] == jnp.arange(experts, dtype=jnp.int32)[None, None, :]
    table = jnp.sum(jnp.where(named, combine[:, :, None], 0.0), axis=1).T
    table, xs, cot = gather_all(table, tokens, cotangent)
    xs = xs.reshape(-1, width)
    scale = lax.dynamic_slice_in_dim(table, lax.axis_index("expert"), 1, axis=1).reshape(-1, 1)
    dys = (scale * cot.reshape(-1, width).astype(jnp.float32)).astype(jnp.bfloat16)
    gate_w = w_gate[0]
    up_w = w_up[0]
    down_w = w_down[0]
    gate = jnp.dot(xs, gate_w, preferred_element_type=jnp.float32)
    upper = jnp.dot(xs, up_w, preferred_element_type=jnp.float32)
    sigma = jax.nn.sigmoid(gate)
    act = (gate * sigma * upper).astype(jnp.bfloat16)
    d_act = contract_cols(dys, down_w)
    d_upper = (d_act * gate * sigma).astype(jnp.bfloat16)
    d_gate = (d_act * upper * sigma * (1.0 + gate * (1.0 - sigma))).astype(jnp.bfloat16)
    part = contract_cols(d_gate, gate_w) + contract_cols(d_upper, up_w)
    token_grad = scatter_sum(part.astype(jnp.bfloat16), rows)
    down_grad = contract_rows(act, dys).astype(jnp.bfloat16)
    gate_grad = contract_rows(xs, d_gate).astype(jnp.bfloat16)
    up_grad = contract_rows(xs, d_upper).astype(jnp.bfloat16)
    return (token_grad, gate_grad[None], up_grad[None], down_grad[None])


def line_order(depth, z):
    def key(p):
        return abs(p - z), -abs(2 * p - depth + 1)

    return sorted(range(depth), key=key)


def pad_to(value, unit):
    return -(-value // unit) * unit


def tiles(total, size):
    full = total // size
    return full, total - full * size


def contract_first(left, right):
    return lax.dot_general(
        left, right, (((0,), (0,)), ((), ())), preferred_element_type=jnp.float32
    )


def fused_kernel(depth, experts, tok, cot, routes, comb, w_gate, w_up, w_down,
                 tg_buf, gg_buf, ug_buf, dg_buf,
                 xs, ct, dys, part, wide, d_raw, dgu, dgu_t, act, act_t, d_act,
                 twin_in, total, x_in, y_in, z_in,
                 tok_buf, route_buf, comb_buf,
                 g_send, g_recv, s_send, s_recv, w_sem, i_sem):
    rows, width = tok.shape
    hid = d_raw.shape[0]
    wpad = xs.shape[1]
    hpad = d_act.shape[1]
    blocks = hpad // 128
    chunk = rows * 8
    z, y, x, c = place()
    t = x * 2 + c
    along, over_y, over_x, twin = peers(depth)
    above, below = (z * 2 + 2 + y, t), (z * 2 - 2 + y, t)
    inward = (jnp.where(z == 0, 1, depth - 2) * 2 + y, t)
    table = [line_order(depth, zz) for zz in range(depth)]

    def plane(i):
        if i == 0:
            return z
        value = 0
        for zz in range(depth):
            value = value + jnp.where(z == zz, table[zz][i], 0)
        return value

    planes = [plane(i) for i in range(depth)]

    def block(p, dy, dx, dc=0):
        yy, xx, cc = (1 - y if dy else y), (1 - x if dx else x), (1 - c if dc else c)
        return (p * 2 + yy) * 4 + xx * 2 + cc

    def at_rows(at, count=rows):
        return pl.ds(pl.multiple_of(at * rows, rows), count)

    bufs = (xs, ct)
    counts = [0, 0]
    apart, far_end = (), False
    side_counts = [[0, 0], [0, 0]]
    group = depth * 5

    barrier = pltpu.get_barrier_semaphore()
    for device in [*along, over_y, over_x, twin]:
        pl.semaphore_signal(barrier, inc=1, device_id=device, device_id_type=MESH)
    me = block(z, 0, 0)
    inputs = [
        pltpu.make_async_copy(src, dst, i_sem.at[k])
        for k, (src, dst) in enumerate(
            ((routes, route_buf), (comb, comb_buf), (tok, tok_buf), (cot, ct.at[at_rows(me)]))
        )
    ]
    for copy in inputs:
        copy.start()
    for side in range(2):
        for j in range(blocks):
            live = min(128, hid - 128 * j)
            if live < 128:
                at = 256 * j + 128 * side
                wide[at + live // 16 * 16 : at + 128, :] = jnp.zeros((128 - live // 16 * 16, width), jnp.bfloat16)
    loads = [pltpu.make_async_copy(w_down.at[0], d_raw, w_sem.at[2 * blocks])]
    for side, weight in ((0, w_gate), (1, w_up)):
        for j in range(blocks):
            live = min(128, hid - 128 * j)
            loads.append(
                pltpu.make_async_copy(
                    weight.at[0, 128 * j : 128 * j + live],
                    wide.at[256 * j + 128 * side : 256 * j + 128 * side + live],
                    w_sem.at[2 * j + side],
                )
            )
    for load in loads:
        load.start()

    for copy in inputs:
        copy.wait()
    lane = lax.broadcasted_iota(jnp.int32, (rows, 128), 1)
    first_lane = width - (wpad - 128)
    owner = lax.rem(lane - first_lane + experts, experts)
    named = jnp.zeros((rows, 128), jnp.float32)
    across = lax.broadcasted_iota(jnp.int32, (rows, rows), 1) == lax.broadcasted_iota(jnp.int32, (rows, rows), 0)
    for k in range(routes.shape[0]):
        chosen = jnp.sum(jnp.where(across, route_buf[k : k + 1, :], 0), axis=1, keepdims=True)
        weight = jnp.sum(jnp.where(across, comb_buf[k : k + 1, :], 0.0), axis=1, keepdims=True)
        named = named + jnp.where(chosen == owner, weight, 0.0)
    high = named.astype(jnp.bfloat16).astype(jnp.float32)
    mid = (named - high).astype(jnp.bfloat16).astype(jnp.float32)
    low = named - high - mid
    piece = jnp.where(lane < first_lane + experts, high, jnp.where(lane < first_lane + 2 * experts, mid, low))
    piece = jnp.where(lane < first_lane + 3 * experts, piece, 0.0)
    tail = jnp.concatenate(
        [tok_buf[:, wpad - 128 : width].astype(jnp.float32), jnp.zeros((rows, wpad - width), jnp.float32)], axis=1
    )
    xs[at_rows(me), : wpad - 128] = tok_buf[:, : wpad - 128]
    xs[at_rows(me), wpad - 128 :] = jnp.where(lane < first_lane, tail, piece).astype(jnp.bfloat16)
    pl.semaphore_wait(barrier, depth + 2)

    def send(q, at, device):
        copy = pltpu.make_async_remote_copy(
            src_ref=bufs[q].at[at_rows(at)],
            dst_ref=bufs[q].at[at_rows(at)],
            send_sem=g_send.at[q, counts[q] // group],
            recv_sem=g_recv.at[q, at],
            device_id=device,
            device_id_type=MESH,
        )
        counts[q] += 1
        copy.start()

    def landed(q, at):
        pltpu.make_async_remote_copy(
            src_ref=bufs[q].at[at_rows(at)],
            dst_ref=bufs[q].at[at_rows(at)],
            send_sem=g_send.at[q, 0],
            recv_sem=g_recv.at[q, at],
            device_id=twin,
            device_id_type=MESH,
        ).wait_recv()

    def send_z(q, i, at):
        if i == 0:
            for device in (inward,) if far_end else (above, below):
                send(q, at, device)
        elif not far_end:
            send(q, at, (jnp.where(planes[i] < z, z + 1, z - 1) * 2 + y, t))

    def first_z(i, q):
        at = block(planes[i], 0, 0)
        if i:
            landed(q, at)
        send_z(q, i, at)
        send(q, at, twin)

    def first_xy(i, q):
        at = block(planes[i], 0, 0)
        send(q, at, over_x)
        send(q, at, over_y)

    def first(i, q):
        first_z(i, q)
        first_xy(i, q)

    def second(i, q):
        by_y, by_x = block(planes[i], 1, 0), block(planes[i], 0, 1)
        near, far, onward = (by_x, by_y, over_y) if q else (by_y, by_x, over_x)
        landed(q, near)
        if i == 0 or apart[i] > ZREACH:
            send(q, near, onward)
        send(q, near, twin)
        landed(q, far)
        send(q, far, twin)

    def third(i, q):
        at = block(planes[i], 1, 1)
        landed(q, at)
        if apart[i] < ZREACH:
            send_z(q, i, at)
        send(q, at, twin)

    def prepare():
        for load in loads:
            load.wait()
        d_act[...] = jnp.zeros(d_act.shape, jnp.float32)

    def here_of(i):
        return pl.ds(pl.multiple_of(planes[i] * chunk, chunk), chunk)

    def scales(i, k):
        for q in range(2):
            landed(q, block(planes[i], k // 2, k % 2, 1))
        first_row = block(planes[i], k // 2, k % 2) - c
        here = at_rows(first_row, 2 * rows)
        spot = lax.broadcasted_iota(jnp.int32, (2 * rows, 128), 1) - first_lane
        e = lax.axis_index("expert")
        mine = (spot == e) | (spot == e + experts) | (spot == e + 2 * experts)
        scale = jnp.sum(jnp.where(mine, xs[here, wpad - 128 :].astype(jnp.float32), 0.0), axis=1, keepdims=True)
        dys[here, :] = (scale * ct[here, :].astype(jnp.float32)).astype(jnp.bfloat16)

    def acts(i):
        d_act[:, :hid] = contract_cols(dys[here_of(i), :], d_raw[...])

    def gates(i):
        here = here_of(i)
        for j in range(blocks):
            both = contract_cols(xs[here, :width], wide[256 * j : 256 * j + 256, :])
            gate, upper = both[:, :128], both[:, 128:]
            da = d_act[:, 128 * j : 128 * j + 128]
            sigma = jax.nn.sigmoid(gate)
            act[here, 128 * j : 128 * j + 128] = (gate * sigma * upper).astype(jnp.bfloat16)
            dgate = da * upper * sigma * (1.0 + gate * (1.0 - sigma))
            dupper = da * gate * sigma
            dgu[here, 256 * j : 256 * j + 128] = dgate.astype(jnp.bfloat16)
            dgu[here, 256 * j + 128 : 256 * j + 256] = dupper.astype(jnp.bfloat16)

    def backs(i, w):
        here = here_of(i)
        for start in range(sides_of[w].start, sides_of[w].stop, 512):
            cols = slice(start, min(start + 512, width))
            part[here, cols] = jnp.dot(
                dgu[here, :], wide[:, cols], preferred_element_type=jnp.float32
            ).astype(jnp.bfloat16)

    def turns(i):
        here = here_of(i)
        for j in range(blocks):
            act_t[128 * j : 128 * j + 128, here] = act[here, 128 * j : 128 * j + 128].T
        for j in range(2 * blocks):
            dgu_t[128 * j : 128 * j + 128, here] = dgu[here, 128 * j : 128 * j + 128].T

    half = rows // 2
    halves = [pl.ds(0, half), pl.ds(half, half)]
    cut = pad_to(width // 2, 512)
    sides_of = (slice(0, cut), slice(cut, width)) if SPLIT else (slice(0, width),)

    def ssend(src, dst, device, w, recv, level=1):
        copy = pltpu.make_async_remote_copy(
            src_ref=src,
            dst_ref=dst,
            send_sem=s_send.at[w, level],
            recv_sem=s_recv.at[w * per_side + recv],
            device_id=device,
            device_id_type=MESH,
        )
        copy.start()
        return copy

    def add(a, b):
        return (a.astype(jnp.float32) + b.astype(jnp.float32)).astype(jnp.bfloat16)

    def both(stage):
        return lambda i, *w: [stage(i, k) for k in (w or range(len(sides_of)))]

    corners = ((1, 1), (0, 1), (1, 0), (0, 0))
    over, last = {}, {}
    z_base = depth * 7
    per_side = depth * 9

    def s0(i, w):
        cols = sides_of[w]
        for dy, dx in corners:
            k = i * 4 + dy * 2 + dx
            ssend(part.at[at_rows(block(planes[i], dy, dx, 1)), cols], twin_in.at[k, :, cols], twin, w, i, 0)

    def merge(h, i, other, w):
        over[h, i, other, w].wait_recv()
        cols = sides_of[w]
        if h == 0:
            k, got = i * 4 + other * 2, x_in[i * 2 + other, :, cols]
        else:
            k, got = i * 4 + other, y_in[i * 2 + other, :, cols]
        total[k, halves[h], cols] = add(total[k, halves[h], cols], got)
        return k

    def s1(i, w):
        cols, base = sides_of[w], depth
        span = twin_in.at[i * 4 : i * 4 + 4, :, cols]
        pltpu.make_async_remote_copy(
            src_ref=span,
            dst_ref=span,
            send_sem=s_send.at[w, 0],
            recv_sem=s_recv.at[w * per_side + i],
            device_id=twin,
            device_id_type=MESH,
        ).wait_recv()
        for dy, dx in corners:
            k = i * 4 + dy * 2 + dx
            total[k, :, cols] = add(part[at_rows(block(planes[i], dy, dx)), cols], twin_in[k, :, cols])
            if dx:
                at = i * 2 + dy
                over[0, i, dy, w] = ssend(
                    total.at[k, halves[0], cols], x_in.at[at, :, cols], over_x, w, base + at
                )
            if dy:
                at = i * 2 + dx
                over[1, i, dx, w] = ssend(
                    total.at[k, halves[1], cols], y_in.at[at, :, cols], over_y, w, base + depth * 2 + at
                )

    def s2(i, w):
        cols, base, at = sides_of[w], depth * 5, depth * 2 + i
        k = merge(0, i, 1, w)
        last[0, i, w] = ssend(total.at[k, halves[0], cols], y_in.at[at, :, cols], over_y, w, base + i)
        k = merge(1, i, 1, w)
        last[1, i, w] = ssend(total.at[k, halves[1], cols], x_in.at[at, :, cols], over_x, w, base + depth + i)

    def s3(i, w):
        cols = sides_of[w]
        for h in range(2):
            k = merge(h, i, 0, w)
            last[h, i, w].wait_recv()
            got = (x_in if h else y_in)[depth * 2 + i, :, cols]
            total[k, halves[h], cols] = add(total[k, halves[h], cols], got)
            if i:
                ssend(
                    total.at[k, halves[h], cols],
                    z_in.at[h * depth + z, :, cols],
                    (planes[i] * 2 + y, t),
                    w,
                    z_base + h * depth + z,
                )

    def finish(w):
        cols = sides_of[w]
        for h in range(2):
            value = total[0, halves[h], cols].astype(jnp.float32)
            for step in range(1, depth):
                at = h * depth + lax.rem(z + step, depth)
                pltpu.make_async_remote_copy(
                    src_ref=total.at[0, halves[h], cols],
                    dst_ref=z_in.at[at, :, cols],
                    send_sem=s_send.at[w, 1],
                    recv_sem=s_recv.at[w * per_side + z_base + at],
                    device_id=twin,
                    device_id_type=MESH,
                ).wait_recv()
                value = value + z_in[at, :, cols].astype(jnp.float32)
            tg_buf[halves[h], cols] = value.astype(jnp.bfloat16)

    msize = 256
    mfull, mrest = tiles(width, msize)

    def wide_tile(cols):
        out = jnp.dot(dgu_t[...], xs[:, cols], preferred_element_type=jnp.float32)
        for j in range(blocks):
            live = min(128, hid - 128 * j)
            for buf, side in ((gg_buf, 0), (ug_buf, 1)):
                at = 256 * j + 128 * side
                buf[128 * j : 128 * j + live, cols] = out[at : at + live].astype(jnp.bfloat16)

    def wide_grads(lo, hi):
        def body(k, _):
            wide_tile(pl.ds(pl.multiple_of(k * msize, msize), msize))
            return 0

        lax.fori_loop(lo, hi, body, 0)

    def wides(k):
        lo, hi = k * mfull // 4, (k + 1) * mfull // 4
        wide_grads(lo, hi)
        if k == 3 and mrest:
            wide_tile(slice(mfull * msize, width))

    nsize = 512
    nfull, nrest = tiles(width, nsize)

    def down():
        def body(k, _):
            cols = pl.ds(pl.multiple_of(k * nsize, nsize), nsize)
            dg_buf[:, cols] = jnp.dot(
                act_t[...], dys[:, cols], preferred_element_type=jnp.float32
            )[:hid].astype(jnp.bfloat16)
            return 0

        lax.fori_loop(0, nfull, body, 0)
        if nrest:
            dg_buf[:, nfull * nsize : width] = jnp.dot(
                act_t[...], dys[:, nfull * nsize : width], preferred_element_type=jnp.float32
            )[:hid].astype(jnp.bfloat16)

    edge = (z == 0) | (z == depth - 1)
    sides = ((edge, tuple(range(depth)), True), (jnp.logical_not(edge), tuple(abs(p - 1) for p in table[1]), False))

    def drain():
        def leave(counts):
            for q in range(2):
                for k in range(0, counts[q], group):
                    span = bufs[q].at[pl.ds(0, min(group, counts[q] - k) * rows)]
                    pltpu.make_async_remote_copy(
                        src_ref=span,
                        dst_ref=span,
                        send_sem=g_send.at[q, k // group],
                        recv_sem=g_recv.at[q, 0],
                        device_id=twin,
                        device_id_type=MESH,
                    ).wait_send()

        for k in range(2):
            pl.when(sides[k][0])(functools.partial(leave, side_counts[k]))
        for w in range(len(sides_of)):
            for k, span in enumerate((twin_in.at[:, :, sides_of[w]], total.at[: depth * 4 - 1, :, sides_of[w]])):
                pltpu.make_async_remote_copy(
                    src_ref=span,
                    dst_ref=span,
                    send_sem=s_send.at[w, k],
                    recv_sem=s_recv.at[0],
                    device_id=twin,
                    device_id_type=MESH,
                ).wait_send()

    stages = {
        "1": first, "2": second, "3": third, "5": first_z, "6": first_xy, "p": prepare, "c": scales, "a": acts, "g": gates,
        "b": both(backs), "s": both(s0), "t": both(s1), "u": both(s2), "v": both(s3), "d": down, "w": wides, "f": finish, "x": turns,
    }

    def walk(steps):
        for step in steps:
            with jax.named_scope(step):
                stages[step[0]](*[int(k) for k in step[1:]])

    def walk_side(k, steps):
        nonlocal apart, far_end
        cond, apart, far_end = sides[k]
        counts[:] = side_counts[k]
        pl.when(cond)(lambda: walk(steps))
        side_counts[k] = counts[:]

    for steps in PLAN:
        if isinstance(steps[0], tuple):
            for k in range(2):
                walk_side(k, steps[k])
        else:
            walk(steps)
    with jax.named_scope("drain"):
        drain()


PLAN = (
    (
        ("100", "101",),
        ("100", "101",),
    ),
    ("p",),
    (
        ("200", "110", "201", "111",),
        ("200", "510", "520", "610", "201", "511", "521", "611", "620", "621",),
    ),
    ("c00", "c01", "c02",),
    (
        ("300", "120", "301", "121",),
        ("530", "531", "300", "301", "630", "631",),
    ),
    ("c03", "a0", "g0", "b0", "s0", "x0",),
    (
        ("210", "211", "130", "131", "310", "311", "220", "221",),
        ("310", "311", "320", "321", "210", "211",),
    ),
    ("c10", "c11", "c12", "c13", "t0", "a1", "g1", "b1", "s1", "x1",),
    (
        ("230", "231", "320", "321",),
        ("220", "221", "330", "331",),
    ),
    ("c20", "c21", "c22", "c23", "u0", "t1", "a2", "g2",),
    (
        ("330", "331",),
        ("230", "231",),
    ),
    ("b2", "s2", "x2",),
    ("c30", "c31", "c32", "c33", "v0", "u1", "t2", "a3", "g3", "v1", "b3", "s3", "u2", "x3"),
    ("t3", "d", "v2", "u3", "w0", "w1", "v3", "w2", "w3", "f0"),
)
ZREACH = 2
SPLIT = 0
VMEM_LIMIT = 54 * 1024 * 1024


def settle_kernel(*refs):
    count = len(refs) // 2
    moves = [
        pltpu.make_async_copy(src, dst, refs[-1].at[k])
        for k, (src, dst) in enumerate(zip(refs[:count], refs[count : 2 * count]))
    ]
    for move in moves:
        move.start()
    for move in moves:
        move.wait()


def settle(*arrays):
    return pl.pallas_call(
        settle_kernel,
        out_shape=[jax.ShapeDtypeStruct(a.shape, a.dtype) for a in arrays],
        in_specs=[pl.BlockSpec(memory_space=pltpu.VMEM)] * len(arrays),
        out_specs=[pl.BlockSpec(memory_space=pl.ANY)] * len(arrays),
        scratch_shapes=[pltpu.SemaphoreType.DMA((len(arrays),))],
        compiler_params=pltpu.CompilerParams(vmem_limit_bytes=8 * 1024 * 1024),
    )(*arrays)


def fused(tokens, cotangent, routes, combine, w_gate, w_up, w_down):
    rows, width = tokens.shape
    hid = w_gate.shape[2]
    groups = lax.axis_size("expert")
    depth = groups // 2
    wpad, hpad = pad_to(width, 128), pad_to(hid, 128)
    count = groups * 4
    everyone = count * rows
    half = rows // 2
    vmem = pl.BlockSpec(memory_space=pltpu.VMEM)
    hbm = pl.BlockSpec(memory_space=pl.ANY)
    bf16, f32 = jnp.bfloat16, jnp.float32
    token_grad, gate_t, up_t, down = pl.pallas_call(
        lambda *refs: fused_kernel(depth, groups, *refs),
        out_shape=[
            pltpu.VMEM(tokens.shape, bf16),
            pltpu.VMEM((hid, width), bf16),
            pltpu.VMEM((hid, width), bf16),
            pltpu.VMEM((hid, width), bf16),
        ],
        in_specs=[hbm] * 7,
        out_specs=[vmem] * 4,
        scratch_shapes=[
            pltpu.VMEM((everyone, wpad), bf16),
            pltpu.VMEM((everyone, width), bf16),
            pltpu.VMEM((everyone, width), bf16),
            pltpu.VMEM((everyone, width), bf16),
            pltpu.VMEM((2 * hpad, width), bf16),
            pltpu.VMEM((hid, width), bf16),
            pltpu.VMEM((everyone, 2 * hpad), bf16),
            pltpu.VMEM((2 * hpad, everyone), bf16),
            pltpu.VMEM((everyone, hpad), bf16),
            pltpu.VMEM((hpad, everyone), bf16),
            pltpu.VMEM((rows * 8, hpad), f32),
            pltpu.VMEM((depth * 4, rows, width), bf16),
            pltpu.VMEM((depth * 4, rows, width), bf16),
            pltpu.VMEM((depth * 3, half, width), bf16),
            pltpu.VMEM((depth * 3, half, width), bf16),
            pltpu.VMEM((depth * 2, half, width), bf16),
            pltpu.VMEM(tokens.shape, bf16),
            pltpu.VMEM(routes.shape[::-1], jnp.int32),
            pltpu.VMEM(combine.shape[::-1], f32),
            pltpu.SemaphoreType.DMA((2, 2)),
            pltpu.SemaphoreType.DMA((2, count)),
            pltpu.SemaphoreType.DMA((1 + SPLIT, 2)),
            pltpu.SemaphoreType.DMA(((1 + SPLIT) * depth * 9,)),
            pltpu.SemaphoreType.DMA((hpad // 64 + 1,)),
            pltpu.SemaphoreType.DMA((4,)),
        ],
        compiler_params=pltpu.CompilerParams(
            collective_id=0, has_side_effects=True, vmem_limit_bytes=VMEM_LIMIT
        ),
    )(
        tokens,
        cotangent,
        routes.T,
        combine.T,
        jnp.swapaxes(w_gate, 1, 2),
        jnp.swapaxes(w_up, 1, 2),
        w_down,
    )
    token_grad, gate_t, up_t, down = settle(token_grad, gate_t, up_t, down)
    return token_grad, jnp.swapaxes(gate_t, 0, 1)[None], jnp.swapaxes(up_t, 0, 1)[None], down[None]


def on_device(tokens, cotangent, routes, combine, w_gate, w_up, w_down):
    groups, shards = lax.axis_size("expert"), lax.axis_size("tensor")
    rows, top_count = routes.shape
    few = w_gate.shape[0] == 1 and groups <= 2 * top_count
    plan = slotted
    if few and shards == 4 and groups % 2 == 0 and rows % 32 == 0:
        plan = fused if groups == 8 and -tokens.shape[1] % 128 >= 3 * groups else dense
    return plan(tokens, cotangent, routes, combine, w_gate, w_up, w_down)


def solution(mesh):
    in_specs = (
        P(("expert", "tensor"), None),
        P(("expert", "tensor"), None),
        P(("expert", "tensor"), None),
        P(("expert", "tensor"), None),
        P("expert", None, "tensor"),
        P("expert", None, "tensor"),
        P("expert", "tensor", None),
    )
    out_specs = (
        P(("expert", "tensor"), None),
        P("expert", None, "tensor"),
        P("expert", None, "tensor"),
        P("expert", "tensor", None),
    )
    return jax.shard_map(
        on_device, mesh=mesh, in_specs=in_specs, out_specs=out_specs, check_vma=False
    )
```

```python
import functools

import jax
import jax.numpy as jnp
from jax import lax
from jax.experimental import pallas as pl
from jax.experimental.pallas import tpu as pltpu
from jax.sharding import PartitionSpec as P

MESH = pl.DeviceIdType.MESH


def route_slots(flat, experts, cap):
    onehot = (flat[:, None] == jnp.arange(experts, dtype=jnp.int32)[None, :]).astype(jnp.int32)
    before = jnp.cumsum(onehot, axis=0) - onehot
    place = jnp.sum(before * onehot, axis=1)
    return flat * cap + place


def contract_rows(left, right):
    return lax.dot_general(
        left, right, (((0,), (0,)), ((), ())), preferred_element_type=jnp.float32
    )


def contract_cols(left, right):
    return lax.dot_general(
        left, right, (((1,), (1,)), ((), ())), preferred_element_type=jnp.float32
    )


def slotted(tokens, cotangent, routes, combine, w_gate, w_up, w_down):
    tok_rows, width = tokens.shape
    top_count = routes.shape[1]
    groups = lax.axis_size("expert")
    experts = groups * w_gate.shape[0]
    cap = max(2, 3 * tok_rows * top_count // (2 * experts))
    flat = routes.reshape(-1)
    slot = route_slots(flat, experts, cap)
    target = jnp.arange(experts * cap, dtype=jnp.int32)
    match = slot[None, :] == target[:, None]
    valid = jnp.any(match, axis=1)
    order = jnp.arange(flat.shape[0], dtype=jnp.int32)
    source = jnp.sum(jnp.where(match, order[None, :], 0), axis=1)
    token = source // top_count
    send_x = jnp.where(valid[:, None], tokens[token], jnp.zeros((), tokens.dtype))
    scaled = combine.reshape(-1)[source][:, None] * cotangent[token].astype(jnp.float32)
    send_dy = jnp.where(valid[:, None], scaled, 0.0).astype(jnp.bfloat16)
    send_x = send_x.reshape(groups, cap, width)
    send_dy = send_dy.reshape(groups, cap, width)
    recv_x, recv_dy = (
        lax.all_to_all(send_x, "expert", split_axis=0, concat_axis=0, tiled=True),
        lax.all_to_all(send_dy, "expert", split_axis=0, concat_axis=0, tiled=True),
    )
    recv_x = recv_x.reshape(groups * cap, width)
    recv_dy = recv_dy.reshape(groups * cap, width)
    xs, dys = (
        lax.all_gather(recv_x, "tensor", axis=0, tiled=True),
        lax.all_gather(recv_dy, "tensor", axis=0, tiled=True),
    )
    gate_w = w_gate[0]
    up_w = w_up[0]
    down_w = w_down[0]
    gate = jnp.dot(xs, gate_w, preferred_element_type=jnp.float32)
    upper = jnp.dot(xs, up_w, preferred_element_type=jnp.float32)
    sigma = jax.nn.sigmoid(gate)
    act = (gate * sigma * upper).astype(jnp.bfloat16)
    d_act = contract_cols(dys, down_w)
    down_grad = contract_rows(act, dys).astype(jnp.bfloat16)
    d_upper = (d_act * gate * sigma).astype(jnp.bfloat16)
    d_gate = (d_act * upper * sigma * (1.0 + gate * (1.0 - sigma))).astype(jnp.bfloat16)
    gate_grad = contract_rows(xs, d_gate).astype(jnp.bfloat16)
    up_grad = contract_rows(xs, d_upper).astype(jnp.bfloat16)
    own = lax.psum_scatter(
        contract_cols(d_gate, gate_w) + contract_cols(d_upper, up_w),
        "tensor",
        scatter_dimension=0,
        tiled=True,
    )
    own = own.astype(jnp.bfloat16).reshape(groups, cap, width)
    back = lax.all_to_all(own, "expert", split_axis=0, concat_axis=0, tiled=True).reshape(
        experts * cap, width
    )
    picked = back[slot].astype(jnp.float32).reshape(tok_rows, top_count, width)
    token_grad = jnp.sum(picked, axis=1).astype(jnp.bfloat16)
    return (token_grad, gate_grad[None], up_grad[None], down_grad[None])


def place():
    e, t = lax.axis_index("expert"), lax.axis_index("tensor")
    return e // 2, lax.rem(e, 2), t // 2, lax.rem(t, 2)


def peers(depth):
    z, y, x, c = place()
    e, t = z * 2 + y, x * 2 + c
    along = [(lax.rem(z + step, depth) * 2 + y, t) for step in range(1, depth)]
    return along, (z * 2 + 1 - y, t), (e, (1 - x) * 2 + c), (e, x * 2 + 1 - c)


def greet(depth):
    along, over_y, over_x, twin = peers(depth)
    barrier = pltpu.get_barrier_semaphore()
    for device in [*along, over_y, over_x, twin]:
        pl.semaphore_signal(barrier, inc=1, device_id=device, device_id_type=MESH)
    pl.semaphore_wait(barrier, depth + 2)


def gather_kernel(depth, s_in, x_in, d_in, s_out, x_out, d_out, send_sem, recv_sem, local_sem):
    z, y, x, c = place()
    along, over_y, over_x, twin = peers(depth)
    ins, outs = (s_in, x_in, d_in), (s_out, x_out, d_out)
    sent = [[], [], []]

    def block(dz, dy, dx, dc=0):
        zz = lax.rem(z + dz, depth)
        yy, xx, cc = (1 - y if dy else y), (1 - x if dx else x), (1 - c if dc else c)
        return (zz * 2 + yy) * 4 + xx * 2 + cc

    def send(p, at, device, first=False):
        copy = pltpu.make_async_remote_copy(
            src_ref=ins[p] if first else outs[p].at[at],
            dst_ref=outs[p].at[at],
            send_sem=send_sem.at[p, len(sent[p])],
            recv_sem=recv_sem.at[p, at],
            device_id=device,
            device_id_type=MESH,
        )
        copy.start()
        sent[p].append(copy)

    def landed(p, at):
        pltpu.make_async_remote_copy(
            src_ref=ins[p],
            dst_ref=outs[p].at[at],
            send_sem=send_sem.at[p, 0],
            recv_sem=recv_sem.at[p, at],
            device_id=twin,
            device_id_type=MESH,
        ).wait_recv()

    me = block(0, 0, 0)
    keep = [pltpu.make_async_copy(ins[p], outs[p].at[me], local_sem.at[p]) for p in range(3)]
    for copy in keep:
        copy.start()
    greet(depth)
    for device in [over_y, over_x, *along, twin]:
        for p in range(3):
            send(p, me, device, True)

    def first_level(dz):
        at = block(dz, 0, 0)
        for p in range(3):
            landed(p, at)
            for device in (over_x, over_y, twin):
                send(p, at, device)

    def second_level(dz):
        by_y, by_x = block(dz, 1, 0), block(dz, 0, 1)
        for p in range(3):
            near, far, onward = (by_x, by_y, over_y) if p == 2 else (by_y, by_x, over_x)
            landed(p, near)
            send(p, near, onward)
            send(p, near, twin)
            landed(p, far)
            send(p, far, twin)

    for dz in range(1, depth):
        first_level(dz)
        second_level(dz - 1)
    second_level(depth - 1)
    for dz in range(depth):
        at = block(dz, 1, 1)
        for p in range(3):
            landed(p, at)
            send(p, at, twin)
    for dz in range(depth):
        for dy in range(2):
            for dx in range(2):
                for p in range(3):
                    landed(p, block(dz, dy, dx, 1))
    for copy in keep:
        copy.wait()
    for p in range(3):
        for copy in sent[p]:
            copy.wait_send()


def gather_all(table, tokens, cotangent):
    count = lax.axis_size("expert") * lax.axis_size("tensor")
    depth = lax.axis_size("expert") // 2
    parts = (table, tokens, cotangent)
    return pl.pallas_call(
        lambda *refs: gather_kernel(depth, *refs),
        out_shape=[jax.ShapeDtypeStruct((count, *a.shape), a.dtype) for a in parts],
        in_specs=[pl.BlockSpec(memory_space=pltpu.VMEM)] * 3,
        out_specs=[pl.BlockSpec(memory_space=pl.ANY)] * 3,
        scratch_shapes=[
            pltpu.SemaphoreType.DMA((3, count - 1)),
            pltpu.SemaphoreType.DMA((3, count)),
            pltpu.SemaphoreType.DMA((3,)),
        ],
        compiler_params=pltpu.CompilerParams(collective_id=0, has_side_effects=True),
    )(*parts)


def scatter_kernel(depth, part, out, total, twin_in, x_in, y_in, z_in, send_sem, recv_sem):
    z, y, x, c = place()
    along, over_y, over_x, twin = peers(depth)
    rows = out.shape[0] // 2
    halves = [pl.ds(0, rows), pl.ds(rows, rows)]
    sent = []

    def block(dz, dy, dx, dc=0):
        zz = lax.rem(z + dz, depth)
        yy, xx, cc = (1 - y if dy else y), (1 - x if dx else x), (1 - c if dc else c)
        return (zz * 2 + yy) * 4 + xx * 2 + cc

    def send(src, dst, device):
        copy = pltpu.make_async_remote_copy(
            src_ref=src,
            dst_ref=dst,
            send_sem=send_sem.at[len(sent)],
            recv_sem=recv_sem.at[len(sent)],
            device_id=device,
            device_id_type=MESH,
        )
        copy.start()
        sent.append(copy)
        return copy

    def add(a, b):
        return (a.astype(jnp.float32) + b.astype(jnp.float32)).astype(jnp.bfloat16)

    steps = [*range(1, depth), 0]
    corners = ((1, 1), (0, 1), (1, 0), (0, 0))
    greet(depth)
    from_twin, over, last, ends = {}, {}, {}, {}
    for dz in steps:
        for dy, dx in corners:
            i = dz * 4 + dy * 2 + dx
            from_twin[i] = send(part.at[block(dz, dy, dx, 1)], twin_in.at[i], twin)

    def merge(half, dz, other):
        over[half, dz, other].wait_recv()
        if half == 0:
            i, got = dz * 4 + other * 2, x_in.at[dz * 2 + other]
        else:
            i, got = dz * 4 + other, y_in.at[dz * 2 + other]
        total[i, halves[half]] = add(total[i, halves[half]], got[...])
        return i

    def first(dz):
        for dy, dx in corners:
            i = dz * 4 + dy * 2 + dx
            from_twin[i].wait_recv()
            total[i] = add(part[block(dz, dy, dx)], twin_in[i])
            if dx:
                over[0, dz, dy] = send(total.at[i, halves[0]], x_in.at[dz * 2 + dy], over_x)
            if dy:
                over[1, dz, dx] = send(total.at[i, halves[1]], y_in.at[dz * 2 + dx], over_y)

    def second(dz):
        i = merge(0, dz, 1)
        last[0, dz] = send(total.at[i, halves[0]], y_in.at[depth * 2 + dz], over_y)
        i = merge(1, dz, 1)
        last[1, dz] = send(total.at[i, halves[1]], x_in.at[depth * 2 + dz], over_x)

    def third(dz):
        for half in range(2):
            i = merge(half, dz, 0)
            last[half, dz].wait_recv()
            got = (x_in if half else y_in)[depth * 2 + dz]
            total[i, halves[half]] = add(total[i, halves[half]], got)
            if dz:
                ends[half, dz] = send(
                    total.at[i, halves[half]], z_in.at[half * (depth - 1) + dz - 1], along[dz - 1]
                )

    for turn in range(depth + 2):
        for stage, lag in ((first, 0), (second, 1), (third, 2)):
            if 0 <= turn - lag < depth:
                stage(steps[turn - lag])
    for half in range(2):
        value = total[0, halves[half]].astype(jnp.float32)
        for dz in range(1, depth):
            ends[half, dz].wait_recv()
            value = value + z_in[half * (depth - 1) + dz - 1].astype(jnp.float32)
        out[halves[half]] = value.astype(jnp.bfloat16)
    for copy in sent:
        copy.wait_send()


def scatter_sum(part, rows):
    width = part.shape[1]
    depth = lax.axis_size("expert") // 2
    copies = depth * 4 + 2 * (depth * 2 + depth + depth - 1)
    half = rows // 2
    return pl.pallas_call(
        lambda *refs: scatter_kernel(depth, *refs),
        out_shape=jax.ShapeDtypeStruct((rows, width), jnp.bfloat16),
        in_specs=[pl.BlockSpec(memory_space=pltpu.VMEM)],
        out_specs=pl.BlockSpec(memory_space=pltpu.VMEM),
        scratch_shapes=[
            pltpu.VMEM((depth * 4, rows, width), jnp.bfloat16),
            pltpu.VMEM((depth * 4, rows, width), jnp.bfloat16),
            pltpu.VMEM((depth * 3, half, width), jnp.bfloat16),
            pltpu.VMEM((depth * 3, half, width), jnp.bfloat16),
            pltpu.VMEM((depth * 2 - 2, half, width), jnp.bfloat16),
            pltpu.SemaphoreType.DMA((copies,)),
            pltpu.SemaphoreType.DMA((copies,)),
        ],
        compiler_params=pltpu.CompilerParams(
            collective_id=1, has_side_effects=True, vmem_limit_bytes=48 * 1024 * 1024
        ),
    )(part.reshape(-1, rows, width))


def dense(tokens, cotangent, routes, combine, w_gate, w_up, w_down):
    rows, width = tokens.shape
    experts = lax.axis_size("expert") * w_gate.shape[0]
    named = routes[:, :, None] == jnp.arange(experts, dtype=jnp.int32)[None, None, :]
    table = jnp.sum(jnp.where(named, combine[:, :, None], 0.0), axis=1).T
    table, xs, cot = gather_all(table, tokens, cotangent)
    xs = xs.reshape(-1, width)
    scale = lax.dynamic_slice_in_dim(table, lax.axis_index("expert"), 1, axis=1).reshape(-1, 1)
    dys = (scale * cot.reshape(-1, width).astype(jnp.float32)).astype(jnp.bfloat16)
    gate_w = w_gate[0]
    up_w = w_up[0]
    down_w = w_down[0]
    gate = jnp.dot(xs, gate_w, preferred_element_type=jnp.float32)
    upper = jnp.dot(xs, up_w, preferred_element_type=jnp.float32)
    sigma = jax.nn.sigmoid(gate)
    act = (gate * sigma * upper).astype(jnp.bfloat16)
    d_act = contract_cols(dys, down_w)
    d_upper = (d_act * gate * sigma).astype(jnp.bfloat16)
    d_gate = (d_act * upper * sigma * (1.0 + gate * (1.0 - sigma))).astype(jnp.bfloat16)
    part = contract_cols(d_gate, gate_w) + contract_cols(d_upper, up_w)
    token_grad = scatter_sum(part.astype(jnp.bfloat16), rows)
    down_grad = contract_rows(act, dys).astype(jnp.bfloat16)
    gate_grad = contract_rows(xs, d_gate).astype(jnp.bfloat16)
    up_grad = contract_rows(xs, d_upper).astype(jnp.bfloat16)
    return (token_grad, gate_grad[None], up_grad[None], down_grad[None])


def line_order(depth, z):
    def key(p):
        return abs(p - z), -abs(2 * p - depth + 1)

    return sorted(range(depth), key=key)


def pad_to(value, unit):
    return -(-value // unit) * unit


def tiles(total, size):
    full = total // size
    return full, total - full * size


def contract_first(left, right):
    return lax.dot_general(
        left, right, (((0,), (0,)), ((), ())), preferred_element_type=jnp.float32
    )


def fused_kernel(depth, experts, tok, cot, routes, comb, w_gate, w_up, w_down,
                 tg_buf, gg_buf, ug_buf, dg_buf,
                 xs, ct, dys, part, wide, d_raw, dgu, dgu_t, act, act_t, d_act,
                 twin_in, total, x_in, y_in, z_in,
                 tok_buf, route_buf, comb_buf,
                 g_send, g_recv, s_send, s_recv, w_sem, i_sem):
    rows, width = tok.shape
    hid = d_raw.shape[0]
    wpad = xs.shape[1]
    hpad = d_act.shape[1]
    blocks = hpad // 128
    chunk = rows * 8
    z, y, x, c = place()
    t = x * 2 + c
    along, over_y, over_x, twin = peers(depth)
    above, below = (z * 2 + 2 + y, t), (z * 2 - 2 + y, t)
    inward = (jnp.where(z == 0, 1, depth - 2) * 2 + y, t)
    table = [line_order(depth, zz) for zz in range(depth)]

    def plane(i):
        if i == 0:
            return z
        value = 0
        for zz in range(depth):
            value = value + jnp.where(z == zz, table[zz][i], 0)
        return value

    planes = [plane(i) for i in range(depth)]

    def block(p, dy, dx, dc=0):
        yy, xx, cc = (1 - y if dy else y), (1 - x if dx else x), (1 - c if dc else c)
        return (p * 2 + yy) * 4 + xx * 2 + cc

    def at_rows(at, count=rows):
        return pl.ds(pl.multiple_of(at * rows, rows), count)

    bufs = (xs, ct)
    counts = [0, 0]
    apart, far_end = (), False
    side_counts = [[0, 0], [0, 0]]
    group = depth * 5

    barrier = pltpu.get_barrier_semaphore()
    for device in [*along, over_y, over_x, twin]:
        pl.semaphore_signal(barrier, inc=1, device_id=device, device_id_type=MESH)
    me = block(z, 0, 0)
    inputs = [
        pltpu.make_async_copy(src, dst, i_sem.at[k])
        for k, (src, dst) in enumerate(
            ((routes, route_buf), (comb, comb_buf), (tok, tok_buf), (cot, ct.at[at_rows(me)]))
        )
    ]
    for copy in inputs:
        copy.start()
    for side in range(2):
        for j in range(blocks):
            live = min(128, hid - 128 * j)
            if live < 128:
                at = 256 * j + 128 * side
                wide[at + live // 16 * 16 : at + 128, :] = jnp.zeros((128 - live // 16 * 16, width), jnp.bfloat16)
    loads = [pltpu.make_async_copy(w_down.at[0], d_raw, w_sem.at[2 * blocks])]
    for side, weight in ((0, w_gate), (1, w_up)):
        for j in range(blocks):
            live = min(128, hid - 128 * j)
            loads.append(
                pltpu.make_async_copy(
                    weight.at[0, 128 * j : 128 * j + live],
                    wide.at[256 * j + 128 * side : 256 * j + 128 * side + live],
                    w_sem.at[2 * j + side],
                )
            )
    for load in loads:
        load.start()

    for copy in inputs:
        copy.wait()
    lane = lax.broadcasted_iota(jnp.int32, (rows, 128), 1)
    first_lane = width - (wpad - 128)
    owner = lax.rem(lane - first_lane + experts, experts)
    named = jnp.zeros((rows, 128), jnp.float32)
    across = lax.broadcasted_iota(jnp.int32, (rows, rows), 1) == lax.broadcasted_iota(jnp.int32, (rows, rows), 0)
    for k in range(routes.shape[0]):
        chosen = jnp.sum(jnp.where(across, route_buf[k : k + 1, :], 0), axis=1, keepdims=True)
        weight = jnp.sum(jnp.where(across, comb_buf[k : k + 1, :], 0.0), axis=1, keepdims=True)
        named = named + jnp.where(chosen == owner, weight, 0.0)
    high = named.astype(jnp.bfloat16).astype(jnp.float32)
    mid = (named - high).astype(jnp.bfloat16).astype(jnp.float32)
    low = named - high - mid
    piece = jnp.where(lane < first_lane + experts, high, jnp.where(lane < first_lane + 2 * experts, mid, low))
    piece = jnp.where(lane < first_lane + 3 * experts, piece, 0.0)
    tail = jnp.concatenate(
        [tok_buf[:, wpad - 128 : width].astype(jnp.float32), jnp.zeros((rows, wpad - width), jnp.float32)], axis=1
    )
    xs[at_rows(me), : wpad - 128] = tok_buf[:, : wpad - 128]
    xs[at_rows(me), wpad - 128 :] = jnp.where(lane < first_lane, tail, piece).astype(jnp.bfloat16)
    pl.semaphore_wait(barrier, depth + 2)

    def send(q, at, device):
        copy = pltpu.make_async_remote_copy(
            src_ref=bufs[q].at[at_rows(at)],
            dst_ref=bufs[q].at[at_rows(at)],
            send_sem=g_send.at[q, counts[q] // group],
            recv_sem=g_recv.at[q, at],
            device_id=device,
            device_id_type=MESH,
        )
        counts[q] += 1
        copy.start()

    def landed(q, at):
        pltpu.make_async_remote_copy(
            src_ref=bufs[q].at[at_rows(at)],
            dst_ref=bufs[q].at[at_rows(at)],
            send_sem=g_send.at[q, 0],
            recv_sem=g_recv.at[q, at],
            device_id=twin,
            device_id_type=MESH,
        ).wait_recv()

    def send_z(q, i, at):
        if i == 0:
            for device in (inward,) if far_end else (above, below):
                send(q, at, device)
        elif not far_end:
            send(q, at, (jnp.where(planes[i] < z, z + 1, z - 1) * 2 + y, t))

    def first_z(i, q):
        at = block(planes[i], 0, 0)
        if i:
            landed(q, at)
        send_z(q, i, at)
        send(q, at, twin)

    def first_xy(i, q):
        at = block(planes[i], 0, 0)
        send(q, at, over_x)
        send(q, at, over_y)

    def first(i, q):
        first_z(i, q)
        first_xy(i, q)

    def second(i, q):
        by_y, by_x = block(planes[i], 1, 0), block(planes[i], 0, 1)
        near, far, onward = (by_x, by_y, over_y) if q else (by_y, by_x, over_x)
        landed(q, near)
        if i == 0 or apart[i] > ZREACH:
            send(q, near, onward)
        send(q, near, twin)
        landed(q, far)
        send(q, far, twin)

    def third(i, q):
        at = block(planes[i], 1, 1)
        landed(q, at)
        if apart[i] < ZREACH:
            send_z(q, i, at)
        send(q, at, twin)

    def prepare():
        for load in loads:
            load.wait()
        d_act[...] = jnp.zeros(d_act.shape, jnp.float32)

    def here_of(i):
        return pl.ds(pl.multiple_of(planes[i] * chunk, chunk), chunk)

    def scales(i, k):
        for q in range(2):
            landed(q, block(planes[i], k // 2, k % 2, 1))
        first_row = block(planes[i], k // 2, k % 2) - c
        here = at_rows(first_row, 2 * rows)
        spot = lax.broadcasted_iota(jnp.int32, (2 * rows, 128), 1) - first_lane
        e = lax.axis_index("expert")
        mine = (spot == e) | (spot == e + experts) | (spot == e + 2 * experts)
        scale = jnp.sum(jnp.where(mine, xs[here, wpad - 128 :].astype(jnp.float32), 0.0), axis=1, keepdims=True)
        dys[here, :] = (scale * ct[here, :].astype(jnp.float32)).astype(jnp.bfloat16)

    def acts(i):
        d_act[:, :hid] = contract_cols(dys[here_of(i), :], d_raw[...])

    def gates(i):
        here = here_of(i)
        for j in range(blocks):
            both = contract_cols(xs[here, :width], wide[256 * j : 256 * j + 256, :])
            gate, upper = both[:, :128], both[:, 128:]
            da = d_act[:, 128 * j : 128 * j + 128]
            sigma = jax.nn.sigmoid(gate)
            act[here, 128 * j : 128 * j + 128] = (gate * sigma * upper).astype(jnp.bfloat16)
            dgate = da * upper * sigma * (1.0 + gate * (1.0 - sigma))
            dupper = da * gate * sigma
            dgu[here, 256 * j : 256 * j + 128] = dgate.astype(jnp.bfloat16)
            dgu[here, 256 * j + 128 : 256 * j + 256] = dupper.astype(jnp.bfloat16)

    def backs(i, w):
        here = here_of(i)
        for start in range(sides_of[w].start, sides_of[w].stop, 512):
            cols = slice(start, min(start + 512, width))
            part[here, cols] = jnp.dot(
                dgu[here, :], wide[:, cols], preferred_element_type=jnp.float32
            ).astype(jnp.bfloat16)

    def turns(i):
        here = here_of(i)
        for j in range(blocks):
            act_t[128 * j : 128 * j + 128, here] = act[here, 128 * j : 128 * j + 128].T
        for j in range(2 * blocks):
            dgu_t[128 * j : 128 * j + 128, here] = dgu[here, 128 * j : 128 * j + 128].T

    half = rows // 2
    halves = [pl.ds(0, half), pl.ds(half, half)]
    cut = pad_to(width // 2, 512)
    sides_of = (slice(0, cut), slice(cut, width)) if SPLIT else (slice(0, width),)

    def ssend(src, dst, device, w, recv, level=1):
        copy = pltpu.make_async_remote_copy(
            src_ref=src,
            dst_ref=dst,
            send_sem=s_send.at[w, level],
            recv_sem=s_recv.at[w * per_side + recv],
            device_id=device,
            device_id_type=MESH,
        )
        copy.start()
        return copy

    def add(a, b):
        return (a.astype(jnp.float32) + b.astype(jnp.float32)).astype(jnp.bfloat16)

    def both(stage):
        return lambda i, *w: [stage(i, k) for k in (w or range(len(sides_of)))]

    corners = ((1, 1), (0, 1), (1, 0), (0, 0))
    over, last = {}, {}
    z_base = depth * 7
    per_side = depth * 9

    def s0(i, w):
        cols = sides_of[w]
        for dy, dx in corners:
            k = i * 4 + dy * 2 + dx
            ssend(part.at[at_rows(block(planes[i], dy, dx, 1)), cols], twin_in.at[k, :, cols], twin, w, i, 0)

    def merge(h, i, other, w):
        over[h, i, other, w].wait_recv()
        cols = sides_of[w]
        if h == 0:
            k, got = i * 4 + other * 2, x_in[i * 2 + other, :, cols]
        else:
            k, got = i * 4 + other, y_in[i * 2 + other, :, cols]
        total[k, halves[h], cols] = add(total[k, halves[h], cols], got)
        return k

    def s1(i, w):
        cols, base = sides_of[w], depth
        span = twin_in.at[i * 4 : i * 4 + 4, :, cols]
        pltpu.make_async_remote_copy(
            src_ref=span,
            dst_ref=span,
            send_sem=s_send.at[w, 0],
            recv_sem=s_recv.at[w * per_side + i],
            device_id=twin,
            device_id_type=MESH,
        ).wait_recv()
        for dy, dx in corners:
            k = i * 4 + dy * 2 + dx
            total[k, :, cols] = add(part[at_rows(block(planes[i], dy, dx)), cols], twin_in[k, :, cols])
            if dx:
                at = i * 2 + dy
                over[0, i, dy, w] = ssend(
                    total.at[k, halves[0], cols], x_in.at[at, :, cols], over_x, w, base + at
                )
            if dy:
                at = i * 2 + dx
                over[1, i, dx, w] = ssend(
                    total.at[k, halves[1], cols], y_in.at[at, :, cols], over_y, w, base + depth * 2 + at
                )

    def s2(i, w):
        cols, base, at = sides_of[w], depth * 5, depth * 2 + i
        k = merge(0, i, 1, w)
        last[0, i, w] = ssend(total.at[k, halves[0], cols], y_in.at[at, :, cols], over_y, w, base + i)
        k = merge(1, i, 1, w)
        last[1, i, w] = ssend(total.at[k, halves[1], cols], x_in.at[at, :, cols], over_x, w, base + depth + i)

    def s3(i, w):
        cols = sides_of[w]
        for h in range(2):
            k = merge(h, i, 0, w)
            last[h, i, w].wait_recv()
            got = (x_in if h else y_in)[depth * 2 + i, :, cols]
            total[k, halves[h], cols] = add(total[k, halves[h], cols], got)
            if i:
                ssend(
                    total.at[k, halves[h], cols],
                    z_in.at[h * depth + z, :, cols],
                    (planes[i] * 2 + y, t),
                    w,
                    z_base + h * depth + z,
                )

    def finish(w):
        cols = sides_of[w]
        for h in range(2):
            value = total[0, halves[h], cols].astype(jnp.float32)
            for step in range(1, depth):
                at = h * depth + lax.rem(z + step, depth)
                pltpu.make_async_remote_copy(
                    src_ref=total.at[0, halves[h], cols],
                    dst_ref=z_in.at[at, :, cols],
                    send_sem=s_send.at[w, 1],
                    recv_sem=s_recv.at[w * per_side + z_base + at],
                    device_id=twin,
                    device_id_type=MESH,
                ).wait_recv()
                value = value + z_in[at, :, cols].astype(jnp.float32)
            tg_buf[halves[h], cols] = value.astype(jnp.bfloat16)

    msize = 256
    mfull, mrest = tiles(width, msize)

    def wide_tile(cols):
        out = jnp.dot(dgu_t[...], xs[:, cols], preferred_element_type=jnp.float32)
        for j in range(blocks):
            live = min(128, hid - 128 * j)
            for buf, side in ((gg_buf, 0), (ug_buf, 1)):
                at = 256 * j + 128 * side
                buf[128 * j : 128 * j + live, cols] = out[at : at + live].astype(jnp.bfloat16)

    def wide_grads(lo, hi):
        def body(k, _):
            wide_tile(pl.ds(pl.multiple_of(k * msize, msize), msize))
            return 0

        lax.fori_loop(lo, hi, body, 0)

    def wides(k):
        lo, hi = k * mfull // 4, (k + 1) * mfull // 4
        wide_grads(lo, hi)
        if k == 3 and mrest:
            wide_tile(slice(mfull * msize, width))

    nsize = 512
    nfull, nrest = tiles(width, nsize)

    def down():
        def body(k, _):
            cols = pl.ds(pl.multiple_of(k * nsize, nsize), nsize)
            dg_buf[:, cols] = jnp.dot(
                act_t[...], dys[:, cols], preferred_element_type=jnp.float32
            )[:hid].astype(jnp.bfloat16)
            return 0

        lax.fori_loop(0, nfull, body, 0)
        if nrest:
            dg_buf[:, nfull * nsize : width] = jnp.dot(
                act_t[...], dys[:, nfull * nsize : width], preferred_element_type=jnp.float32
            )[:hid].astype(jnp.bfloat16)

    edge = (z == 0) | (z == depth - 1)
    sides = ((edge, tuple(range(depth)), True), (jnp.logical_not(edge), tuple(abs(p - 1) for p in table[1]), False))

    def drain():
        def leave(counts):
            for q in range(2):
                for k in range(0, counts[q], group):
                    span = bufs[q].at[pl.ds(0, min(group, counts[q] - k) * rows)]
                    pltpu.make_async_remote_copy(
                        src_ref=span,
                        dst_ref=span,
                        send_sem=g_send.at[q, k // group],
                        recv_sem=g_recv.at[q, 0],
                        device_id=twin,
                        device_id_type=MESH,
                    ).wait_send()

        for k in range(2):
            pl.when(sides[k][0])(functools.partial(leave, side_counts[k]))
        for w in range(len(sides_of)):
            for k, span in enumerate((twin_in.at[:, :, sides_of[w]], total.at[: depth * 4 - 1, :, sides_of[w]])):
                pltpu.make_async_remote_copy(
                    src_ref=span,
                    dst_ref=span,
                    send_sem=s_send.at[w, k],
                    recv_sem=s_recv.at[0],
                    device_id=twin,
                    device_id_type=MESH,
                ).wait_send()

    stages = {
        "1": first, "2": second, "3": third, "5": first_z, "6": first_xy, "p": prepare, "c": scales, "a": acts, "g": gates,
        "b": both(backs), "s": both(s0), "t": both(s1), "u": both(s2), "v": both(s3), "d": down, "w": wides, "f": finish, "x": turns,
    }

    def walk(steps):
        for step in steps:
            with jax.named_scope(step):
                stages[step[0]](*[int(k) for k in step[1:]])

    def walk_side(k, steps):
        nonlocal apart, far_end
        cond, apart, far_end = sides[k]
        counts[:] = side_counts[k]
        pl.when(cond)(lambda: walk(steps))
        side_counts[k] = counts[:]

    for steps in PLAN:
        if isinstance(steps[0], tuple):
            for k in range(2):
                walk_side(k, steps[k])
        else:
            walk(steps)
    with jax.named_scope("drain"):
        drain()


PLAN = (
    (
        ("100", "101",),
        ("100", "101",),
    ),
    ("p",),
    (
        ("200", "110", "201", "111",),
        ("200", "510", "520", "610", "201", "511", "521", "611", "620", "621",),
    ),
    ("c00", "c01", "c02",),
    (
        ("300", "120", "301", "121",),
        ("530", "531", "300", "301", "630", "631",),
    ),
    ("c03", "a0", "g0", "b0", "s0", "x0",),
    (
        ("210", "211", "130", "131", "310", "311", "220", "221",),
        ("310", "311", "320", "321", "210", "211",),
    ),
    ("c10", "c11", "c12", "c13", "t0", "a1", "g1", "b1", "s1", "x1",),
    (
        ("230", "231", "320", "321",),
        ("220", "221", "330", "331",),
    ),
    ("c20", "c21", "c22", "c23", "u0", "t1", "a2", "g2",),
    (
        ("330", "331",),
        ("230", "231",),
    ),
    ("b2", "s2", "x2",),
    ("c30", "c31", "c32", "c33", "v0", "u1", "t2", "a3", "g3", "b3", "s3", "v1", "u2", "x3"),
    ("t3", "d", "v2", "u3", "w0", "w1", "v3", "w2", "w3", "f0"),
)
ZREACH = 2
SPLIT = 0
VMEM_LIMIT = 54 * 1024 * 1024


def settle_kernel(*refs):
    count = len(refs) // 2
    moves = [
        pltpu.make_async_copy(src, dst, refs[-1].at[k])
        for k, (src, dst) in enumerate(zip(refs[:count], refs[count : 2 * count]))
    ]
    for move in moves:
        move.start()
    for move in moves:
        move.wait()


def settle(*arrays):
    return pl.pallas_call(
        settle_kernel,
        out_shape=[jax.ShapeDtypeStruct(a.shape, a.dtype) for a in arrays],
        in_specs=[pl.BlockSpec(memory_space=pltpu.VMEM)] * len(arrays),
        out_specs=[pl.BlockSpec(memory_space=pl.ANY)] * len(arrays),
        scratch_shapes=[pltpu.SemaphoreType.DMA((len(arrays),))],
        compiler_params=pltpu.CompilerParams(vmem_limit_bytes=8 * 1024 * 1024),
    )(*arrays)


def fused(tokens, cotangent, routes, combine, w_gate, w_up, w_down):
    rows, width = tokens.shape
    hid = w_gate.shape[2]
    groups = lax.axis_size("expert")
    depth = groups // 2
    wpad, hpad = pad_to(width, 128), pad_to(hid, 128)
    count = groups * 4
    everyone = count * rows
    half = rows // 2
    vmem = pl.BlockSpec(memory_space=pltpu.VMEM)
    hbm = pl.BlockSpec(memory_space=pl.ANY)
    bf16, f32 = jnp.bfloat16, jnp.float32
    token_grad, gate_t, up_t, down = pl.pallas_call(
        lambda *refs: fused_kernel(depth, groups, *refs),
        out_shape=[
            pltpu.VMEM(tokens.shape, bf16),
            pltpu.VMEM((hid, width), bf16),
            pltpu.VMEM((hid, width), bf16),
            pltpu.VMEM((hid, width), bf16),
        ],
        in_specs=[hbm] * 7,
        out_specs=[vmem] * 4,
        scratch_shapes=[
            pltpu.VMEM((everyone, wpad), bf16),
            pltpu.VMEM((everyone, width), bf16),
            pltpu.VMEM((everyone, width), bf16),
            pltpu.VMEM((everyone, width), bf16),
            pltpu.VMEM((2 * hpad, width), bf16),
            pltpu.VMEM((hid, width), bf16),
            pltpu.VMEM((everyone, 2 * hpad), bf16),
            pltpu.VMEM((2 * hpad, everyone), bf16),
            pltpu.VMEM((everyone, hpad), bf16),
            pltpu.VMEM((hpad, everyone), bf16),
            pltpu.VMEM((rows * 8, hpad), f32),
            pltpu.VMEM((depth * 4, rows, width), bf16),
            pltpu.VMEM((depth * 4, rows, width), bf16),
            pltpu.VMEM((depth * 3, half, width), bf16),
            pltpu.VMEM((depth * 3, half, width), bf16),
            pltpu.VMEM((depth * 2, half, width), bf16),
            pltpu.VMEM(tokens.shape, bf16),
            pltpu.VMEM(routes.shape[::-1], jnp.int32),
            pltpu.VMEM(combine.shape[::-1], f32),
            pltpu.SemaphoreType.DMA((2, 2)),
            pltpu.SemaphoreType.DMA((2, count)),
            pltpu.SemaphoreType.DMA((1 + SPLIT, 2)),
            pltpu.SemaphoreType.DMA(((1 + SPLIT) * depth * 9,)),
            pltpu.SemaphoreType.DMA((hpad // 64 + 1,)),
            pltpu.SemaphoreType.DMA((4,)),
        ],
        compiler_params=pltpu.CompilerParams(
            collective_id=0, has_side_effects=True, vmem_limit_bytes=VMEM_LIMIT
        ),
    )(
        tokens,
        cotangent,
        routes.T,
        combine.T,
        jnp.swapaxes(w_gate, 1, 2),
        jnp.swapaxes(w_up, 1, 2),
        w_down,
    )
    token_grad, gate_t, up_t, down = settle(token_grad, gate_t, up_t, down)
    return token_grad, jnp.swapaxes(gate_t, 0, 1)[None], jnp.swapaxes(up_t, 0, 1)[None], down[None]


def on_device(tokens, cotangent, routes, combine, w_gate, w_up, w_down):
    groups, shards = lax.axis_size("expert"), lax.axis_size("tensor")
    rows, top_count = routes.shape
    few = w_gate.shape[0] == 1 and groups <= 2 * top_count
    plan = slotted
    if few and shards == 4 and groups % 2 == 0 and rows % 32 == 0:
        plan = fused if groups == 8 and -tokens.shape[1] % 128 >= 3 * groups else dense
    return plan(tokens, cotangent, routes, combine, w_gate, w_up, w_down)


def solution(mesh):
    in_specs = (
        P(("expert", "tensor"), None),
        P(("expert", "tensor"), None),
        P(("expert", "tensor"), None),
        P(("expert", "tensor"), None),
        P("expert", None, "tensor"),
        P("expert", None, "tensor"),
        P("expert", "tensor", None),
    )
    out_specs = (
        P(("expert", "tensor"), None),
        P("expert", None, "tensor"),
        P("expert", None, "tensor"),
        P("expert", "tensor", None),
    )
    return jax.shard_map(
        on_device, mesh=mesh, in_specs=in_specs, out_specs=out_specs, check_vma=False
    )
```
